256 devices in a mesh: gz: 256 (over y, z, x, core).
Axes of the slice: x: 4, y: 4, z: 8, core: 2. Of those that a mesh axis runs over, the one named last changes fastest.
Arguments:
- state: float32 [8, 256, 64, 256], P(None, 'gz'), may hold values from -18 to 18
- explicit_rhs: float32 [2, 8, 256, 64, 256], P(None, None, 'gz'), may hold values from -6 to 6
- implicit_rhs: float32 [2, 8, 256, 64, 256], P(None, None, 'gz'), may hold values from -6 to 6
- implicit_coef: float32 [8], replicated, may hold values from 0.5 to 4
Outputs:
- section_value: float32 [8, 256, 64, 256], P(None, 'gz')
- weighted_rms: float32 [], replicated
The draws below stay inside these ranges and needn't reach their ends.
All inputs are finite; a program needn't handle non-finite values.
Results may differ from the reference program's by a relative error of at most 0.0001.
Values sent between devices are 32-bit elements; how exact they have to be, the bound alone decides.
A program may use at most 64 MiB of HBM per device.

```python
import math
import jax
import jax.numpy as jnp
from jax import lax

S = 8
NY = 64
NX = 256
ITERS = 3
NZ = 256


def draw_state(key, part):
    depth = jnp.arange(NZ, dtype=jnp.float32) / NZ
    amplitude = (1.0 + 2.0 * depth)[None, :, None, None]
    noise = jnp.clip(jax.random.normal(key, (S, NZ, NY, NX), jnp.float32), -6.0, 6.0)
    return noise * amplitude


def shard_levels(own_key, dims, shards, smallest, high):
    factor_of = 1.0
    for position, shards_of in shards:
        steps = jax.random.uniform(jax.random.fold_in(jax.random.fold_in(own_key, 6), position), (shards_of,), jnp.float32, smallest / len(shards), high / len(shards))
        factor_of = factor_of * jnp.repeat(jnp.exp(steps), dims[position] // shards_of).reshape((-1,) + (1,) * (len(dims) - 1 - position))
    return factor_of


def scatter_about(key, extent, width, most, cuts=(), kind=jnp.bfloat16):
    factor_of = shard_levels(key, extent, cuts, -0.22, 0.18) if cuts else 1.0
    values = jax.random.normal(key, extent, jnp.float32) * width * factor_of
    return jnp.minimum(jnp.maximum(values, -most), most).astype(kind)


def setup_inputs(seed: int = 0) -> dict:
    keys = jax.random.split(jax.random.key(seed), 5)
    state = draw_state(jax.random.fold_in(keys[4], 71), 0)
    explicit_rhs = scatter_about(keys[1], (2, S, NZ, NY, NX), 1.0, 6.0, ((2, 256),), jnp.float32)
    implicit_rhs = scatter_about(keys[2], (2, S, NZ, NY, NX), 1.0, 6.0, ((2, 256),), jnp.float32)
    implicit_coef = jnp.clip(jnp.exp(jax.random.uniform(keys[3], (S,), jnp.float32, math.log(0.5), math.log(4.0))), 0.5, 4.0)
    return dict(state=state, explicit_rhs=explicit_rhs, implicit_rhs=implicit_rhs, implicit_coef=implicit_coef)


explicit_weights = (5535828885825.0 / 10492691773637.0, 788022342437.0 / 10882634858940.0)
implicit_weights = (2746238789719.0 / 10658868560708.0, -640167445237.0 / 6845629431997.0)

def operate(field, implicit_coef):
    flat = jnp.pad(field, ((0, 0), (0, 0), (1, 1), (1, 1)))
    beside = jnp.roll(field, 1, axis=1) + jnp.roll(field, -1, axis=1)
    beside = beside + flat[:, :, 2:, 1:-1] + flat[:, :, :-2, 1:-1] + flat[:, :, 1:-1, 2:] + flat[:, :, 1:-1, :-2]
    return field - implicit_coef[:, None, None, None] * (beside - 6.0 * field)

def species_sum(first, second):
    return lax.optimization_barrier(jnp.sum(first * second, axis=(1, 2, 3)))

def widen(values):
    return values[:, None, None, None]

def reference(state, explicit_rhs, implicit_rhs, implicit_coef):
    section_in = state + explicit_weights[0] * explicit_rhs[0] + explicit_weights[1] * explicit_rhs[1]
    section_in = section_in + implicit_weights[0] * implicit_rhs[0] + implicit_weights[1] * implicit_rhs[1]
    solution = section_in
    residual = section_in - operate(section_in, implicit_coef)
    direction = residual
    norm_now = species_sum(residual, residual)
    for iteration in range(ITERS):
        image = operate(direction, implicit_coef)
        step_size = norm_now / species_sum(direction, image)
        solution = solution + widen(step_size) * direction
        residual = residual - widen(step_size) * image
        if iteration + 1 < ITERS:
            norm_next = species_sum(residual, residual)
            direction = residual + widen(norm_next / norm_now) * direction
            norm_now = norm_next
    scaled = (solution - section_in) / (1.0 + 0.1 * jnp.abs(state))
    weighted_rms = jnp.sqrt(jnp.sum(scaled * scaled) / (S * NZ * NY * NX))
    return (solution, weighted_rms)
```

```python
import functools

import jax
import jax.numpy as jnp
from jax import lax
from jax.experimental import pallas as pl
from jax.experimental.pallas import tpu as pltpu
from jax.sharding import Mesh
from jax.sharding import PartitionSpec as P

AXES = ("gz_0", "gz_1", "gz_2", "gz_3")
MESH = pl.DeviceIdType.MESH

explicit_weights = (5535828885825.0 / 10492691773637.0, 788022342437.0 / 10882634858940.0)
implicit_weights = (2746238789719.0 / 10658868560708.0, -640167445237.0 / 6845629431997.0)

HALO = 4
RING = 8
MOMENTS = 6
SHIFT = 8.0


def remote(src, dst, send, recv, device):
    return pltpu.make_async_remote_copy(
        src_ref=src,
        dst_ref=dst,
        send_sem=send,
        recv_sem=recv,
        device_id=device,
        device_id_type=MESH,
    )


def laplace(below, here, above, shift=0.0):
    ny, nx = here.shape
    row = lax.broadcasted_iota(jnp.int32, here.shape, 0)
    lane = lax.broadcasted_iota(jnp.int32, here.shape, 1)
    beside = below + above
    beside = beside + jnp.where(row == ny - 1, 0.0, pltpu.roll(here, ny - 1, 0))
    beside = beside + jnp.where(row == 0, 0.0, pltpu.roll(here, 1, 0))
    beside = beside + jnp.where(lane == nx - 1, 0.0, pltpu.roll(here, nx - 1, 1))
    beside = beside + jnp.where(lane == 0, 0.0, pltpu.roll(here, 1, 1))
    return (6.0 - shift) * here - beside


def folded(value):
    total = value[0:8]
    for at in range(8, value.shape[0], 8):
        total = total + value[at : at + 8]
    return total


def row_of(sums):
    lane = lax.broadcasted_iota(jnp.int32, (1, 128), 1)
    row = jnp.zeros((1, 128), jnp.float32)
    for k, value in enumerate(sums):
        row = jnp.where(lane == k, jnp.sum(value, axis=(0, 1), keepdims=True), row)
    return row


def entries(row, count):
    lane = lax.broadcasted_iota(jnp.int32, (1, 128), 1)
    return [
        jnp.sum(jnp.where(lane == k, row, 0.0), axis=1, keepdims=True) for k in range(count)
    ]


def basis_steps(nu, c):
    diagonal = 1.0 + SHIFT * c

    def gram(p, shift):
        total = None
        for i, a in enumerate(p):
            for j, b in enumerate(p):
                term = a * b * nu[i + j + shift]
                total = term if total is None else total + term
        return total

    def step(norm, along):
        energy = jnp.maximum(diagonal * gram(along, 0) + c * gram(along, 1), norm)
        return jnp.where(norm > 0.0, norm / energy, 0.0)

    norm = nu[0]
    first = norm / (diagonal * nu[0] + c * nu[1])
    residual = (1.0 - first * diagonal, -first * c)
    norm_next = jnp.maximum(gram(residual, 0), 0.0)
    ratio = norm_next / norm
    along = (residual[0] + ratio, residual[1])
    second = step(norm_next, along)
    norm = norm_next
    image = (diagonal * along[0], diagonal * along[1] + c * along[0], c * along[1])
    residual = (
        residual[0] - second * image[0],
        residual[1] - second * image[1],
        -second * image[2],
    )
    norm_next = jnp.maximum(gram(residual, 0), 0.0)
    ratio = jnp.where(norm > 0.0, norm_next / norm, 0.0)
    last = (residual[0] + ratio * along[0], residual[1] + ratio * along[1], residual[2])
    third = step(norm_next, last)
    return (
        -c * (first + second * along[0] + third * last[0]),
        -c * (second * along[1] + third * last[1]),
        -c * (third * last[2]),
    )


def kernel(
    sizes,
    cells,
    state,
    explicit,
    implicit,
    coef,
    u_out,
    rms_out,
    state_in,
    explicit_in,
    implicit_in,
    b_send,
    d_send,
    field,
    weight,
    v0,
    v1,
    v2,
    u_send,
    u_home,
    relay,
    rows,
    own_rows,
    in_sem,
    out_sem,
    send_sem,
    relay_send,
    recv_sem,
    relay_recv,
    halo_send,
    halo_recv,
    row_send,
    row_recv,
):
    count_y, count_z = sizes
    groups = count_y * count_z
    y, z, x, core = (lax.axis_index(a) for a in AXES)
    place = 2 * x + core
    group = y * count_z + z
    right, left, across = lax.rem(x + 1, 4), lax.rem(x + 3, 4), lax.rem(x + 2, 4)

    def at(of_group, of_x, of_core):
        return (of_group // count_z, lax.rem(of_group, count_z), of_x, of_core)

    def in_ring(of_x, of_core):
        return (y, z, of_x, of_core)

    order = (
        (across, 0),
        (across, 1),
        (right, 0),
        (left, 0),
        (right, 1),
        (left, 1),
        (x, 1 - core),
        (x, core),
    )

    loads = []
    for k, (ox, oc) in enumerate(order):
        s = 2 * ox + oc
        loads.append(
            (
                pltpu.make_async_copy(state.at[s, 0], state_in.at[k], in_sem.at[k, 0]),
                pltpu.make_async_copy(explicit.at[:, s, 0], explicit_in.at[k], in_sem.at[k, 1]),
                pltpu.make_async_copy(implicit.at[:, s, 0], implicit_in.at[k], in_sem.at[k, 2]),
            )
        )
        for copy in loads[-1]:
            copy.start()

    barrier = pltpu.get_barrier_semaphore()

    def greet_far(k, _):
        other = lax.rem(group + k, groups)
        pl.semaphore_signal(
            barrier, inc=1, device_id=at(other, x, core), device_id_type=MESH
        )
        return _

    def greet_near(k, _):
        other = lax.rem(place + k, RING)
        pl.semaphore_signal(
            barrier,
            inc=1,
            device_id=in_ring(other // 2, lax.rem(other, 2)),
            device_id_type=MESH,
        )
        return _

    lax.fori_loop(1, RING, greet_near, 0)
    lax.fori_loop(1, groups, greet_far, 0)
    pl.semaphore_wait(barrier, groups - 1 + RING - 1)

    sent = []

    def spread(phase, k, source, target):
        if k < 2:
            copy = remote(
                source,
                relay.at[phase, k],
                send_sem.at[phase, k],
                relay_recv.at[phase, k],
                in_ring(right if k == 0 else left, core),
            )
        else:
            copy = remote(
                source,
                target,
                send_sem.at[phase, k],
                recv_sem.at[phase, place],
                in_ring(*order[k]),
            )
        copy.start()
        sent.append(copy)

    def forward(phase, target):
        for k in range(2):
            origin = 2 * (left if k == 0 else right) + core
            slot = relay.at[phase, k]
            pltpu.make_async_remote_copy(
                slot, slot, send_sem.at[phase, k], relay_recv.at[phase, k],
                device_id=in_ring(right, core), device_id_type=MESH,
            ).wait_recv()
            copy = remote(
                slot,
                target(origin),
                relay_send.at[phase, k],
                recv_sem.at[phase, origin],
                in_ring(right if k == 0 else left, k),
            )
            copy.start()
            sent.append(copy)

    def arrived(phase, target, origin):
        slot = target(origin)
        pltpu.make_async_remote_copy(
            slot, slot, send_sem.at[phase, 0], recv_sem.at[phase, origin],
            device_id=in_ring(right, core), device_id_type=MESH,
        ).wait_recv()

    def in_field(origin):
        return field.at[HALO + origin]

    def in_weight(origin):
        return weight.at[origin]

    def at_home(origin):
        return u_home.at[origin]

    def pass_on(origin):
        side = 2 * (origin // HALO) - 1
        slot = lax.rem(origin + HALO + RING, HALO + RING + HALO)
        copy = remote(
            field.at[HALO + origin],
            field.at[slot],
            halo_send.at[origin],
            halo_recv.at[slot],
            at(lax.rem(group + side + groups, groups), x, core),
        )
        copy.start()
        sent.append(copy)

    for k in range(RING):
        for copy in loads[k]:
            copy.wait()
        b = (
            state_in[k]
            + explicit_weights[0] * explicit_in[k, 0]
            + explicit_weights[1] * explicit_in[k, 1]
        )
        b = b + implicit_weights[0] * implicit_in[k, 0] + implicit_weights[1] * implicit_in[k, 1]
        if k < RING - 1:
            b_send[k] = b
            spread(0, k, b_send.at[k], in_field(place))
        else:
            field[HALO + place] = b
            pass_on(place)
    forward(0, in_field)
    for k in range(RING):
        d = 1.0 / (1.0 + 0.1 * jnp.abs(state_in[k]))
        if k < RING - 1:
            d_send[k] = d * d
            spread(1, k, d_send.at[k], in_weight(place))
        else:
            weight[place] = d * d
    for ox, oc in (order[6], order[2], order[3], order[4], order[5], order[0], order[1]):
        origin = 2 * ox + oc
        arrived(0, in_field, origin)
        pass_on(origin)
    forward(1, in_weight)
    for slot in (*range(HALO), *range(HALO + RING, HALO + RING + HALO)):
        place_of = field.at[slot]
        pltpu.make_async_remote_copy(
            place_of, place_of, halo_send.at[0], halo_recv.at[slot],
            device_id=in_ring(right, core), device_id_type=MESH,
        ).wait_recv()

    last = 2 * HALO + RING - 1
    low, high = HALO, HALO + RING

    def plane(ref, j, shift):
        return laplace(ref[j - 1], ref[j], ref[j + 1], shift)

    def first_pass(j, _):
        v0[j] = plane(field, j, 0.0)
        return _

    lax.fori_loop(1, last, first_pass, 0)

    def edge_pass(source, target):
        def body(j, _):
            target[j] = plane(source, j, SHIFT)
            return _

        return body

    def dot_pass(source, target):
        def body(j, sums):
            here = source[j]
            image = plane(source, j, SHIFT)
            if target is not None:
                target[j] = image
            return (sums[0] + folded(here * here), sums[1] + folded(here * image))

        return body

    zero = jnp.zeros((8, field.shape[-1]), jnp.float32)
    sums = []
    lax.fori_loop(2, low, edge_pass(v0, v1), 0)
    sums += lax.fori_loop(low, high, dot_pass(v0, v1), (zero, zero))
    lax.fori_loop(high, last - 1, edge_pass(v0, v1), 0)
    lax.fori_loop(3, low, edge_pass(v1, v2), 0)
    sums += lax.fori_loop(low, high, dot_pass(v1, v2), (zero, zero))
    lax.fori_loop(high, last - 2, edge_pass(v1, v2), 0)
    sums += lax.fori_loop(low, high, dot_pass(v2, None), (zero, zero))

    def publish(phase, values):
        row = row_of(values)
        own_rows[phase] = row
        rows[phase, group] = row

        def send(k, _):
            other = lax.rem(group + k, groups)
            remote(
                own_rows.at[phase],
                rows.at[phase, group],
                row_send.at[phase],
                row_recv.at[phase],
                at(other, x, core),
            ).start()
            return _

        lax.fori_loop(1, groups, send, 0)

    def total(phase, count):
        others = rows.at[phase, pl.ds(0, count - 1)]
        pltpu.make_async_remote_copy(
            others, others, row_send.at[phase], row_recv.at[phase],
            device_id=in_ring(right, core), device_id_type=MESH,
        ).wait_recv()
        row = rows[phase, 0]
        for k in range(1, count):
            row = row + rows[phase, k]
        return row

    def rows_sent(phase, count):
        others = rows.at[phase, pl.ds(0, count - 1)]
        pltpu.make_async_remote_copy(
            others, others, row_send.at[phase], row_recv.at[phase],
            device_id=in_ring(right, core), device_id_type=MESH,
        ).wait_send()

    publish(0, sums)

    for ox, oc in order[:7]:
        arrived(1, in_weight, 2 * ox + oc)

    def weighted(j, sums):
        d = weight[j - low]
        a, b, e = v0[j], v1[j], v2[j]
        da, db, de = d * a, d * b, d * e
        products = (da * a, da * b, da * e, db * b, db * e, de * e)
        return tuple(total + folded(product) for total, product in zip(sums, products))

    publish(1, lax.fori_loop(low, high, weighted, (zero,) * 6))

    c = coef[place]
    nu = entries(total(0, groups), MOMENTS)
    factor = basis_steps(nu, c)

    for k, (ox, oc) in enumerate(order):
        q = 2 * ox + oc
        j = low + q
        u = field[j] + (factor[0] * v0[j] + (factor[1] * v1[j] + factor[2] * v2[j]))
        if k < RING - 1:
            u_send[k] = u
            spread(2, k, u_send.at[k], at_home(place))
        else:
            u_home[place] = u

    out = []

    def write(s):
        copy = pltpu.make_async_copy(u_home.at[s], u_out.at[s, 0], out_sem.at[s])
        copy.start()
        out.append(copy)

    write(place)
    forward(2, at_home)

    g = entries(total(1, groups), 6)
    own = (
        factor[0] * factor[0] * g[0]
        + factor[1] * factor[1] * g[3]
        + factor[2] * factor[2] * g[5]
        + 2.0 * (factor[0] * factor[1] * g[1] + factor[0] * factor[2] * g[2] + factor[1] * factor[2] * g[4])
    )
    row = jnp.broadcast_to(own, (1, 128))
    own_rows[2] = row
    rows[2, place] = row

    def send_last(k, _):
        other = lax.rem(place + k, RING)
        remote(
            own_rows.at[2],
            rows.at[2, place],
            row_send.at[2],
            row_recv.at[2],
            in_ring(other // 2, lax.rem(other, 2)),
        ).start()
        return _

    lax.fori_loop(1, RING, send_last, 0)

    for ox, oc in (order[6], order[2], order[3], order[4], order[5], order[0], order[1]):
        s = 2 * ox + oc
        arrived(2, at_home, s)
        write(s)

    rms_out[...] = jnp.sqrt(total(2, RING)[0:1, 0:1] / cells)
    for copy in out:
        copy.wait()
    for copy in sent:
        copy.wait_send()
    rows_sent(0, groups)
    rows_sent(1, groups)
    rows_sent(2, RING)


def shards(state, explicit_rhs, implicit_rhs, implicit_coef):
    species, _, ny, nx = state.shape
    sizes = (lax.axis_size(AXES[0]), lax.axis_size(AXES[1]))
    groups = sizes[0] * sizes[1]
    cells = species * ny * nx * groups * RING
    depth = RING + 2 * HALO
    f32 = jnp.float32
    any_space = pl.BlockSpec(memory_space=pl.ANY)
    dma = pltpu.SemaphoreType.DMA
    u, rms = pl.pallas_call(
        functools.partial(kernel, sizes, cells),
        out_shape=(
            jax.ShapeDtypeStruct(state.shape, f32),
            jax.ShapeDtypeStruct((1, 1), f32),
        ),
        in_specs=[any_space] * 3 + [pl.BlockSpec(memory_space=pltpu.SMEM)],
        out_specs=(any_space, pl.BlockSpec(memory_space=pltpu.VMEM)),
        scratch_shapes=[
            pltpu.VMEM((RING, ny, nx), f32),
            pltpu.VMEM((RING, 2, ny, nx), f32),
            pltpu.VMEM((RING, 2, ny, nx), f32),
            pltpu.VMEM((RING, ny, nx), f32),
            pltpu.VMEM((RING, ny, nx), f32),
            pltpu.VMEM((depth, ny, nx), f32),
            pltpu.VMEM((RING, ny, nx), f32),
            pltpu.VMEM((depth, ny, nx), f32),
            pltpu.VMEM((depth, ny, nx), f32),
            pltpu.VMEM((depth, ny, nx), f32),
            pltpu.VMEM((RING, ny, nx), f32),
            pltpu.VMEM((RING, ny, nx), f32),
            pltpu.VMEM((3, 2, ny, nx), f32),
            pltpu.VMEM((3, max(groups, RING), 1, 128), f32),
            pltpu.VMEM((3, 1, 128), f32),
            dma((RING, 3)),
            dma((RING,)),
            dma((3, RING)),
            dma((3, 2)),
            dma((3, RING)),
            dma((3, 2)),
            dma((RING,)),
            dma((depth,)),
            dma((3,)),
            dma((3,)),
        ],
        compiler_params=pltpu.CompilerParams(collective_id=0, has_side_effects=True),
        name="section",
    )(state, explicit_rhs, implicit_rhs, implicit_coef)
    return u, rms[0, 0]


def solution(mesh):
    torus = Mesh(mesh.devices.reshape(-1, 8, 4, 2), AXES)
    placed = (
        P(None, AXES, None, None),
        P(None, None, AXES, None, None),
        P(None, None, AXES, None, None),
        P(),
    )
    return jax.shard_map(
        shards,
        mesh=torus,
        in_specs=placed,
        out_specs=(P(None, AXES, None, None), P()),
        check_vma=False,
    )
```

```python
import functools

import jax
import jax.numpy as jnp
from jax import lax
from jax.experimental import pallas as pl
from jax.experimental.pallas import tpu as pltpu
from jax.sharding import Mesh
from jax.sharding import PartitionSpec as P

AXES = ("gz_0", "gz_1", "gz_2", "gz_3")
MESH = pl.DeviceIdType.MESH

explicit_weights = (5535828885825.0 / 10492691773637.0, 788022342437.0 / 10882634858940.0)
implicit_weights = (2746238789719.0 / 10658868560708.0, -640167445237.0 / 6845629431997.0)

HALO = 4
RING = 8
MOMENTS = 6
SHIFT = 8.0


def remote(src, dst, send, recv, device):
    return pltpu.make_async_remote_copy(
        src_ref=src,
        dst_ref=dst,
        send_sem=send,
        recv_sem=recv,
        device_id=device,
        device_id_type=MESH,
    )


def laplace(below, here, above, shift=0.0):
    ny, nx = here.shape
    row = lax.broadcasted_iota(jnp.int32, here.shape, 0)
    lane = lax.broadcasted_iota(jnp.int32, here.shape, 1)
    beside = below + above
    beside = beside + jnp.where(row == ny - 1, 0.0, pltpu.roll(here, ny - 1, 0))
    beside = beside + jnp.where(row == 0, 0.0, pltpu.roll(here, 1, 0))
    beside = beside + jnp.where(lane == nx - 1, 0.0, pltpu.roll(here, nx - 1, 1))
    beside = beside + jnp.where(lane == 0, 0.0, pltpu.roll(here, 1, 1))
    return (6.0 - shift) * here - beside


def folded(value):
    total = value[0:8]
    for at in range(8, value.shape[0], 8):
        total = total + value[at : at + 8]
    return total


def row_of(sums):
    row = lax.broadcasted_iota(jnp.int32, (8, 128), 0)
    lane = lax.broadcasted_iota(jnp.int32, (8, 128), 1)
    stacked = jnp.zeros((8, 128), jnp.float32)
    for k, value in enumerate(sums):
        halves = sum(value[:, at : at + 128] for at in range(0, value.shape[1], 128))
        stacked = jnp.where(row == k, jnp.sum(halves, axis=0, keepdims=True), stacked)
    each = jnp.where(row == lane, jnp.sum(stacked, axis=1, keepdims=True), 0.0)
    return jnp.sum(each, axis=0, keepdims=True)


def entries(row, count):
    lane = lax.broadcasted_iota(jnp.int32, (1, 128), 1)
    return [
        jnp.sum(jnp.where(lane == k, row, 0.0), axis=1, keepdims=True) for k in range(count)
    ]


def basis_steps(nu, c):
    diagonal = 1.0 + SHIFT * c

    def gram(p, shift):
        total = None
        for i, a in enumerate(p):
            for j, b in enumerate(p):
                term = a * b * nu[i + j + shift]
                total = term if total is None else total + term
        return total

    def step(norm, along):
        energy = jnp.maximum(diagonal * gram(along, 0) + c * gram(along, 1), norm)
        return jnp.where(norm > 0.0, norm / energy, 0.0)

    norm = nu[0]
    first = norm / (diagonal * nu[0] + c * nu[1])
    residual = (1.0 - first * diagonal, -first * c)
    norm_next = jnp.maximum(gram(residual, 0), 0.0)
    ratio = norm_next / norm
    along = (residual[0] + ratio, residual[1])
    second = step(norm_next, along)
    norm = norm_next
    image = (diagonal * along[0], diagonal * along[1] + c * along[0], c * along[1])
    residual = (
        residual[0] - second * image[0],
        residual[1] - second * image[1],
        -second * image[2],
    )
    norm_next = jnp.maximum(gram(residual, 0), 0.0)
    ratio = jnp.where(norm > 0.0, norm_next / norm, 0.0)
    last = (residual[0] + ratio * along[0], residual[1] + ratio * along[1], residual[2])
    third = step(norm_next, last)
    return (
        -c * (first + second * along[0] + third * last[0]),
        -c * (second * along[1] + third * last[1]),
        -c * (third * last[2]),
    )


def kernel(
    sizes,
    cells,
    state,
    explicit,
    implicit,
    coef,
    u_home,
    rms_out,
    state_in,
    explicit_in,
    implicit_in,
    coef_in,
    b_send,
    d_send,
    field,
    weight,
    v0,
    v1,
    v2,
    u_send,
    relay,
    rows,
    own_rows,
    in_sem,
    send_sem,
    relay_send,
    recv_sem,
    relay_recv,
    halo_send,
    halo_recv,
    row_send,
    row_recv,
    wave_sem,
):
    count_y, count_z = sizes
    groups = count_y * count_z
    y, z, x, core = (lax.axis_index(a) for a in AXES)
    place = 2 * x + core
    group = y * count_z + z
    right, left, across = lax.rem(x + 1, 4), lax.rem(x + 3, 4), lax.rem(x + 2, 4)

    def in_ring(of_x, of_core):
        return (y, z, of_x, of_core)

    def at_group(step):
        of_group = lax.rem(group + step + groups, groups)
        return (of_group // count_z, lax.rem(of_group, count_z), x, core)

    def away(step_y, step_z):
        return (lax.rem(y + step_y, count_y), lax.rem(z + step_z + count_z, count_z), x, core)

    partners = [(x, 1 - core)] + [
        (chip, c) for chip in (right, left, across) for c in (core, 1 - core)
    ]

    barrier = pltpu.get_barrier_semaphore()
    near = [in_ring(*p) for p in partners] + [at_group(1), at_group(-1)]
    near += [away(k, 0) for k in range(1, count_y)] + [away(0, 1), away(0, -1)]
    for device in near:
        pl.semaphore_signal(barrier, inc=1, device_id=device, device_id_type=MESH)

    loads = [
        pltpu.make_async_copy(state.at[:, 0], state_in, in_sem.at[0]),
        pltpu.make_async_copy(explicit.at[:, :, 0], explicit_in, in_sem.at[1]),
        pltpu.make_async_copy(implicit.at[:, :, 0], implicit_in, in_sem.at[2]),
        pltpu.make_async_copy(coef, coef_in, in_sem.at[3]),
    ]
    for copy in loads:
        copy.start()
    for copy in loads:
        copy.wait()

    def prepare(s, _):
        b = (
            state_in[s]
            + explicit_weights[0] * explicit_in[0, s]
            + explicit_weights[1] * explicit_in[1, s]
        )
        b_send[s] = b + (
            implicit_weights[0] * implicit_in[0, s] + implicit_weights[1] * implicit_in[1, s]
        )
        d = 1.0 / (1.0 + 0.1 * jnp.abs(state_in[s]))
        d_send[s] = d * d
        return _

    lax.fori_loop(0, RING, prepare, 0, unroll=2)
    field[HALO + place] = b_send[place]
    weight[place] = d_send[place]

    pl.semaphore_wait(barrier, len(near))

    waves = [[(0, 1), (0, -1)], [(0, 2), (0, -2)], [(0, 4)]]

    def wave(k):
        for step in waves[k]:
            pl.semaphore_signal(
                wave_sem.at[k], inc=1, device_id=away(*step), device_id_type=MESH
            )

    def after_wave(k):
        pl.semaphore_wait(wave_sem.at[k], len(waves[k]))

    wave(0)
    sent = []

    def issue(*args):
        copy = remote(*args)
        copy.start()
        sent.append(copy)

    def direct(phase, block, target, chip, c):
        number = 2 * chip + c
        issue(
            block(number),
            target.at[place],
            send_sem.at[phase, number],
            recv_sem.at[phase, place],
            in_ring(chip, c),
        )

    def first_leg(phase, block):
        for k, chip in ((0, right), (1, left)):
            number = 2 * across + k
            issue(
                block(number),
                relay.at[phase, k],
                send_sem.at[phase, number],
                relay_recv.at[phase, k],
                in_ring(chip, core),
            )

    def second_leg(phase, target):
        for k, source, chip in ((0, left, right), (1, right, left)):
            slot = relay.at[phase, k]
            origin = 2 * source + core
            remote(
                slot, slot, relay_send.at[phase, k], relay_recv.at[phase, k], in_ring(right, core)
            ).wait_recv()
            issue(
                slot,
                target.at[origin],
                relay_send.at[phase, k],
                recv_sem.at[phase, origin],
                in_ring(chip, k),
            )

    def spread(phase, block, target, between=None):
        first_leg(phase, block)
        direct(phase, block, target, x, 1 - core)
        direct(phase, block, target, right, core)
        direct(phase, block, target, left, core)
        if between is not None:
            between()

    def spread_rest(phase, block, target):
        direct(phase, block, target, right, 1 - core)
        direct(phase, block, target, left, 1 - core)

    def arrived(phase, target, chip, c):
        origin = 2 * chip + c
        slot = target.at[origin]
        remote(
            slot, slot, send_sem.at[phase, 0], recv_sem.at[phase, origin], in_ring(right, core)
        ).wait_recv()
        return origin

    own_planes = field.at[pl.ds(HALO, RING)]

    def pass_on(origin):
        side = 2 * (origin // HALO) - 1
        slot = lax.rem(origin + HALO + RING, HALO + RING + HALO)
        issue(
            own_planes.at[origin],
            field.at[slot],
            halo_send.at[origin],
            halo_recv.at[slot],
            at_group(side),
        )

    arrivals = (partners[0], partners[1], partners[3], partners[5], partners[6], partners[2], partners[4])

    spread(0, lambda n: b_send.at[n], own_planes, lambda: pass_on(place))
    second_leg(0, own_planes)
    spread_rest(0, lambda n: b_send.at[n], own_planes)
    spread(1, lambda n: d_send.at[n], weight)
    spread_rest(1, lambda n: d_send.at[n], weight)
    after_wave(0)
    wave(1)
    for chip, c in arrivals:
        pass_on(arrived(0, own_planes, chip, c))
    after_wave(1)
    wave(2)
    second_leg(1, weight)

    last = 2 * HALO + RING
    low, high = HALO, HALO + RING

    def planes(source, target, shift, start, stop):
        def body(j, _):
            target[j] = laplace(source[j - 1], source[j], source[j + 1], shift)
            return _

        lax.fori_loop(start, stop, body, 0, unroll=True)

    planes(field, v0, 0.0, low + 1, high - 1)
    planes(v0, v1, SHIFT, low + 2, high - 2)
    planes(v1, v2, SHIFT, low + 3, high - 3)
    for slot in (*range(low), *range(high, last)):
        place_of = field.at[slot]
        remote(
            place_of, place_of, halo_send.at[0], halo_recv.at[slot], in_ring(right, core)
        ).wait_recv()
    for depth, (source, target, shift) in enumerate(
        ((field, v0, 0.0), (v0, v1, SHIFT), (v1, v2, SHIFT)), 1
    ):
        planes(source, target, shift, depth, low + depth)
        planes(source, target, shift, high - depth, last - depth)

    zero = jnp.zeros((8, field.shape[-1]), jnp.float32)

    def moments(j, sums):
        a, b, e = v0[j], v1[j], v2[j]
        image = laplace(v2[j - 1], e, v2[j + 1], SHIFT)
        products = (a * a, a * b, b * b, b * e, e * e, e * image)
        return tuple(total + folded(product) for total, product in zip(sums, products))

    sums = lax.fori_loop(low, high, moments, (zero,) * MOMENTS, unroll=2)

    far = sorted(
        ((dy, dz) for dy in range(count_y) for dz in range(count_z) if (dy, dz) != (0, 0)),
        key=lambda d: -min(d[0], count_y - d[0]) - min(d[1], count_z - d[1]),
    )

    def publish(phase, values):
        row = row_of(values)
        own_rows[phase] = row
        rows[phase, group] = row
        for step in far:
            remote(
                own_rows.at[phase],
                rows.at[phase, group],
                row_send.at[phase],
                row_recv.at[phase],
                away(*step),
            ).start()

    def others(phase, count):
        some = rows.at[phase, pl.ds(0, count - 1)]
        return remote(
            some, some, row_send.at[phase], row_recv.at[phase], in_ring(right, core)
        )

    def total(phase, count):
        others(phase, count).wait_recv()
        parts = [rows[phase, k] for k in range(count)]
        while len(parts) > 1:
            parts = [a + b for a, b in zip(parts[::2], parts[1::2])]
        return parts[0]

    after_wave(2)
    publish(0, sums)

    for chip, c in arrivals:
        arrived(1, weight, chip, c)

    def weighted(j, sums):
        d = weight[j - low]
        a, b, e = v0[j], v1[j], v2[j]
        da, db, de = d * a, d * b, d * e
        products = (da * a, da * b, da * e, db * b, db * e, de * e)
        return tuple(total + folded(product) for total, product in zip(sums, products))

    publish(1, lax.fori_loop(low, high, weighted, (zero,) * MOMENTS, unroll=2))

    c = coef_in[place]
    nu = entries(total(0, groups), MOMENTS)
    factor = basis_steps(nu, c)

    def update(k, _):
        j = low + k
        u = field[j] + (factor[0] * v0[j] + (factor[1] * v1[j] + factor[2] * v2[j]))
        u_send[k] = u
        return _

    lax.fori_loop(0, RING, update, 0, unroll=2)
    u_home[place] = u_send[place]
    spread(2, lambda n: u_send.at[n], u_home)
    spread_rest(2, lambda n: u_send.at[n], u_home)
    second_leg(2, u_home)

    g = entries(total(1, groups), MOMENTS)
    own = (
        factor[0] * factor[0] * g[0]
        + factor[1] * factor[1] * g[3]
        + factor[2] * factor[2] * g[5]
        + 2.0 * (factor[0] * factor[1] * g[1] + factor[0] * factor[2] * g[2] + factor[1] * factor[2] * g[4])
    )
    row = jnp.broadcast_to(own, (1, 128))
    own_rows[2] = row
    rows[2, place] = row
    for p in partners:
        remote(
            own_rows.at[2], rows.at[2, place], row_send.at[2], row_recv.at[2], in_ring(*p)
        ).start()
    rms_out[...] = jnp.sqrt(total(2, RING)[0:1, 0:1] / cells)

    for chip, c in arrivals:
        arrived(2, u_home, chip, c)
    for copy in sent:
        copy.wait_send()
    others(0, groups).wait_send()
    others(1, groups).wait_send()
    others(2, RING).wait_send()


def shards(state, explicit_rhs, implicit_rhs, implicit_coef):
    species, _, ny, nx = state.shape
    sizes = (lax.axis_size(AXES[0]), lax.axis_size(AXES[1]))
    groups = sizes[0] * sizes[1]
    cells = species * ny * nx * groups * RING
    depth = RING + 2 * HALO
    f32 = jnp.float32
    hbm, vmem = (pl.BlockSpec(memory_space=m) for m in (pltpu.HBM, pltpu.VMEM))
    dma = pltpu.SemaphoreType.DMA
    u, rms = pl.pallas_call(
        functools.partial(kernel, sizes, cells),
        out_shape=(
            jax.ShapeDtypeStruct((species, ny, nx), f32),
            jax.ShapeDtypeStruct((1, 1), f32),
        ),
        in_specs=[hbm] * 4,
        out_specs=(vmem, vmem),
        scratch_shapes=[
            pltpu.VMEM((RING, ny, nx), f32),
            pltpu.VMEM((2, RING, ny, nx), f32),
            pltpu.VMEM((2, RING, ny, nx), f32),
            pltpu.SMEM((species,), f32),
            pltpu.VMEM((RING, ny, nx), f32),
            pltpu.VMEM((RING, ny, nx), f32),
            pltpu.VMEM((depth, ny, nx), f32),
            pltpu.VMEM((RING, ny, nx), f32),
            pltpu.VMEM((depth, ny, nx), f32),
            pltpu.VMEM((depth, ny, nx), f32),
            pltpu.VMEM((depth, ny, nx), f32),
            pltpu.VMEM((RING, ny, nx), f32),
            pltpu.VMEM((3, 2, ny, nx), f32),
            pltpu.VMEM((3, max(groups, RING), 1, 128), f32),
            pltpu.VMEM((3, 1, 128), f32),
            dma((4,)),
            dma((3, RING)),
            dma((3, 2)),
            dma((3, RING)),
            dma((3, 2)),
            dma((RING,)),
            dma((depth,)),
            dma((3,)),
            dma((3,)),
            pltpu.SemaphoreType.REGULAR((3,)),
        ],
        compiler_params=pltpu.CompilerParams(
            collective_id=0, has_side_effects=True, vmem_limit_bytes=24 * 2**20
        ),
        name="section",
    )(
        *(
            pltpu.with_memory_space_constraint(a, pltpu.HBM)
            for a in (state, explicit_rhs, implicit_rhs, implicit_coef)
        )
    )
    return u.reshape(state.shape), rms[0, 0]


def solution(mesh):
    torus = Mesh(mesh.devices.reshape(-1, 8, 4, 2), AXES)
    placed = (
        P(None, AXES, None, None),
        P(None, None, AXES, None, None),
        P(None, None, AXES, None, None),
        P(),
    )
    return jax.shard_map(
        shards,
        mesh=torus,
        in_specs=placed,
        out_specs=(P(None, AXES, None, None), P()),
        check_vma=False,
    )
```

```python
import functools

import jax
import jax.numpy as jnp
from jax import lax
from jax.experimental import pallas as pl
from jax.experimental.pallas import tpu as pltpu
from jax.sharding import Mesh
from jax.sharding import PartitionSpec as P

AXES = ("gz_0", "gz_1", "gz_2", "gz_3")
MESH = pl.DeviceIdType.MESH

explicit_weights = (5535828885825.0 / 10492691773637.0, 788022342437.0 / 10882634858940.0)
implicit_weights = (2746238789719.0 / 10658868560708.0, -640167445237.0 / 6845629431997.0)

HALO = 4
RING = 8
MOMENTS = 6
SHIFT = 8.0
EARLY = 24


def remote(src, dst, send, recv, device):
    return pltpu.make_async_remote_copy(
        src_ref=src,
        dst_ref=dst,
        send_sem=send,
        recv_sem=recv,
        device_id=device,
        device_id_type=MESH,
    )


def laplace(below, here, above, shift=0.0):
    ny, nx = here.shape
    row = lax.broadcasted_iota(jnp.int32, here.shape, 0)
    lane = lax.broadcasted_iota(jnp.int32, here.shape, 1)
    beside = below + above
    beside = beside + jnp.where(row == ny - 1, 0.0, pltpu.roll(here, ny - 1, 0))
    beside = beside + jnp.where(row == 0, 0.0, pltpu.roll(here, 1, 0))
    beside = beside + jnp.where(lane == nx - 1, 0.0, pltpu.roll(here, nx - 1, 1))
    beside = beside + jnp.where(lane == 0, 0.0, pltpu.roll(here, 1, 1))
    return (6.0 - shift) * here - beside


def folded(value):
    total = value[0:8]
    for at in range(8, value.shape[0], 8):
        total = total + value[at : at + 8]
    return total


def row_of(sums):
    row = lax.broadcasted_iota(jnp.int32, (8, 128), 0)
    lane = lax.broadcasted_iota(jnp.int32, (8, 128), 1)
    stacked = jnp.zeros((8, 128), jnp.float32)
    for k, value in enumerate(sums):
        halves = sum(value[:, at : at + 128] for at in range(0, value.shape[1], 128))
        stacked = jnp.where(row == k, jnp.sum(halves, axis=0, keepdims=True), stacked)
    each = jnp.where(row == lane, jnp.sum(stacked, axis=1, keepdims=True), 0.0)
    return jnp.sum(each, axis=0, keepdims=True)


def entries(row, count):
    lane = lax.broadcasted_iota(jnp.int32, (1, 128), 1)
    return [
        jnp.sum(jnp.where(lane == k, row, 0.0), axis=1, keepdims=True) for k in range(count)
    ]


def basis_steps(nu, c):
    diagonal = 1.0 + SHIFT * c

    def gram(p, shift):
        total = None
        for i, a in enumerate(p):
            for j, b in enumerate(p):
                term = a * b * nu[i + j + shift]
                total = term if total is None else total + term
        return total

    def step(norm, along):
        energy = jnp.maximum(diagonal * gram(along, 0) + c * gram(along, 1), norm)
        return jnp.where(norm > 0.0, norm / energy, 0.0)

    norm = nu[0]
    first = norm / (diagonal * nu[0] + c * nu[1])
    residual = (1.0 - first * diagonal, -first * c)
    norm_next = jnp.maximum(gram(residual, 0), 0.0)
    ratio = norm_next / norm
    along = (residual[0] + ratio, residual[1])
    second = step(norm_next, along)
    norm = norm_next
    image = (diagonal * along[0], diagonal * along[1] + c * along[0], c * along[1])
    residual = (
        residual[0] - second * image[0],
        residual[1] - second * image[1],
        -second * image[2],
    )
    norm_next = jnp.maximum(gram(residual, 0), 0.0)
    ratio = jnp.where(norm > 0.0, norm_next / norm, 0.0)
    last = (residual[0] + ratio * along[0], residual[1] + ratio * along[1], residual[2])
    third = step(norm_next, last)
    return (
        -c * (first + second * along[0] + third * last[0]),
        -c * (second * along[1] + third * last[1]),
        -c * (third * last[2]),
    )


def kernel(
    sizes,
    cells,
    state,
    explicit,
    implicit,
    coef,
    u_home,
    rms_out,
    state_in,
    explicit_in,
    implicit_in,
    coef_in,
    b_send,
    d_send,
    field,
    weight,
    v0,
    v1,
    v2,
    v_home,
    u_send,
    rows,
    own_rows,
    factors,
    in_sem,
    b_recv,
    halo_recv,
    sent_sem,
    recv_sem,
    row_sent,
    row_recv,
    wave_sem,
):
    count_y, count_z = sizes
    groups = count_y * count_z
    ny = field.shape[1]
    y, z, x, core = (lax.axis_index(a) for a in AXES)
    place = 2 * x + core
    group = y * count_z + z
    right, left, across = lax.rem(x + 1, 4), lax.rem(x + 3, 4), lax.rem(x + 2, 4)

    def in_ring(chip, c):
        return (y, z, chip, c)

    def at_group(step):
        of_group = lax.rem(group + step + groups, groups)
        return (of_group // count_z, lax.rem(of_group, count_z), x, core)

    def away(step_y, step_z):
        return (lax.rem(y + step_y, count_y), lax.rem(z + step_z + count_z, count_z), x, core)

    partner = (x, 1 - core)
    outside = [(chip, c) for c in (core, 1 - core) for chip in (across, right, left)]
    partners = [partner] + outside

    barrier = pltpu.get_barrier_semaphore()
    near = [in_ring(*p) for p in partners] + [at_group(1), at_group(-1)]
    near += [away(k, 0) for k in range(1, count_y)] + [away(0, 1), away(0, -1)]
    for device in near:
        pl.semaphore_signal(barrier, inc=1, device_id=device, device_id_type=MESH)

    for k, chip in enumerate((across, right, left, x)):
        pair = pl.ds(2 * chip, 2)
        for source, target in (
            (state.at[pair, 0], state_in.at[pair]),
            (explicit.at[:, pair, 0], explicit_in.at[:, pair]),
            (implicit.at[:, pair, 0], implicit_in.at[:, pair]),
        ):
            pltpu.make_async_copy(source, target, in_sem.at[k]).start()
    coef_load = pltpu.make_async_copy(coef, coef_in, in_sem.at[4])
    coef_load.start()

    def section_in(k, chip):
        ten = field.at[pl.ds(0, 10)]
        pltpu.make_async_copy(ten, ten, in_sem.at[k]).wait()
        for s in (2 * chip, 2 * chip + 1):
            b = (
                state_in[s]
                + explicit_weights[0] * explicit_in[0, s]
                + explicit_weights[1] * explicit_in[1, s]
            )
            b_send[s] = b + (
                implicit_weights[0] * implicit_in[0, s]
                + implicit_weights[1] * implicit_in[1, s]
            )

    BLOCK, HALO_BLOCK, WEIGHT, EARLY_ROWS, FACTORS, LATE_ROWS = range(6)

    def issue(source, target, kind, recv, device):
        remote(source, target, sent_sem.at[kind], recv, device).start()

    def some_copies(of, kind, recv):
        return remote(of, of, sent_sem.at[kind], recv, in_ring(right, core))

    def send_b(chip, c):
        issue(
            b_send.at[2 * chip + c],
            field.at[HALO + place],
            BLOCK,
            b_recv.at[place],
            in_ring(chip, c),
        )

    def pass_on(origin):
        half = origin // HALO
        issue(
            field.at[HALO + origin],
            field.at[lax.rem(origin + HALO + RING, HALO + RING + HALO)],
            HALO_BLOCK,
            halo_recv.at[1 - half],
            at_group(2 * half - 1),
        )

    def b_arrived(chip, c):
        origin = 2 * chip + c
        some_copies(field.at[HALO + origin], BLOCK, b_recv.at[origin]).wait_recv()
        return origin

    section_in(0, across)
    pl.semaphore_wait(barrier, len(near))
    send_b(across, core)
    send_b(across, 1 - core)
    section_in(1, right)
    send_b(right, core)
    section_in(2, left)
    send_b(left, core)
    section_in(3, x)
    field[HALO + place] = b_send[place]
    send_b(*partner)
    send_b(right, 1 - core)
    send_b(left, 1 - core)
    pass_on(place)

    waves = [[(0, 1), (0, -1)], [(0, 2), (0, -2)], [(0, 4)]]

    def wave(k):
        for step in waves[k]:
            pl.semaphore_signal(
                wave_sem.at[k], inc=1, device_id=away(*step), device_id_type=MESH
            )

    def after_wave(k):
        pl.semaphore_wait(wave_sem.at[k], len(waves[k]))

    wave(0)

    def weigh(s, _):
        d = 1.0 / (1.0 + 0.1 * jnp.abs(state_in[s]))
        d_send[s] = d * d
        return _

    lax.fori_loop(0, RING, weigh, 0, unroll=2)
    weight[place] = d_send[place]
    pass_on(b_arrived(*partner))
    for chip, c in partners:
        number = 2 * chip + c
        issue(
            d_send.at[number],
            weight.at[place],
            WEIGHT,
            recv_sem.at[WEIGHT],
            in_ring(chip, c),
        )
    for number, p in enumerate(
        (
            (across, core),
            (across, 1 - core),
            (right, core),
            (left, core),
            (right, 1 - core),
            (left, 1 - core),
        )
    ):
        pass_on(b_arrived(*p))
        if number == 1:
            after_wave(0)
            wave(1)
    after_wave(1)
    wave(2)

    last = 2 * HALO + RING
    low, high = HALO, HALO + RING

    def planes(source, target, shift, start, stop):
        def body(j, _):
            target[j] = laplace(source[j - 1], source[j], source[j + 1], shift)
            return _

        lax.fori_loop(start, stop, body, 0, unroll=True)

    planes(field, v0, 0.0, low + 1, high - 1)
    planes(v0, v1, SHIFT, low + 2, high - 2)
    planes(v1, v2, SHIFT, low + 3, high - 3)
    zero = jnp.zeros((8, field.shape[-1]), jnp.float32)

    def moments(j, sums):
        a, b, e = v0[j], v1[j], v2[j]
        image = laplace(v2[j - 1], e, v2[j + 1], SHIFT)
        products = (a * a, a * b, b * b, b * e, e * e, e * image)
        return tuple(total + folded(product) for total, product in zip(sums, products))

    sums = (zero,) * MOMENTS
    middle = low + RING // 2
    for side, start, stop in (
        (0, lambda d: d, lambda d: low + d),
        (1, lambda d: high - d, lambda d: last - d),
    ):
        four = field.at[pl.ds(side * high, HALO)]
        some_copies(four, HALO_BLOCK, halo_recv.at[side]).wait_recv()
        planes(field, v0, 0.0, start(1), stop(1))
        planes(v0, v1, SHIFT, start(2), stop(2))
        planes(v1, v2, SHIFT, start(3), stop(3))
        if side == 0:
            sums = lax.fori_loop(low, middle, moments, sums, unroll=2)

    for chip, c in outside + [partner]:
        number = 2 * chip + c
        for i, v in enumerate((v0, v1, v2)):
            issue(
                v.at[low + number, pl.ds(0, EARLY)],
                v_home.at[place, i],
                EARLY_ROWS,
                recv_sem.at[EARLY_ROWS],
                in_ring(chip, c),
            )

    sums = lax.fori_loop(middle, high, moments, sums, unroll=2)

    far = sorted(
        ((dy, dz) for dy in range(count_y) for dz in range(count_z) if (dy, dz) != (0, 0)),
        key=lambda d: -min(d[0], count_y - d[0]) - min(d[1], count_z - d[1]),
    )

    def publish(phase, values):
        row = row_of(values)
        own_rows[phase] = row
        rows[phase, group] = row
        for step in far:
            remote(
                own_rows.at[phase],
                rows.at[phase, group],
                row_sent.at[phase],
                row_recv.at[phase],
                away(*step),
            ).start()

    def others(phase, count):
        some = rows.at[phase, pl.ds(0, count - 1)]
        return remote(
            some, some, row_sent.at[phase], row_recv.at[phase], in_ring(right, core)
        )

    def total(phase, count):
        others(phase, count).wait_recv()
        parts = [rows[phase, k] for k in range(count)]
        while len(parts) > 1:
            parts = [a + b for a, b in zip(parts[::2], parts[1::2])]
        return parts[0]

    after_wave(2)
    publish(0, sums)

    seven = pl.ds(0, RING - 1)
    everything = {
        BLOCK: b_send.at[seven],
        HALO_BLOCK: field.at[pl.ds(0, RING)],
        WEIGHT: weight.at[seven],
        EARLY_ROWS: v_home.at[seven],
        FACTORS: factors.at[seven],
        LATE_ROWS: u_send.at[seven],
    }

    def all_copies(kind):
        return some_copies(everything[kind], kind, recv_sem.at[kind])

    all_copies(WEIGHT).wait_recv()

    def weighted(j, sums):
        d = weight[j - low]
        a, b, e = v0[j], v1[j], v2[j]
        da, db, de = d * a, d * b, d * e
        products = (da * a, da * b, da * e, db * b, db * e, de * e)
        return tuple(total + folded(product) for total, product in zip(sums, products))

    publish(1, lax.fori_loop(low, high, weighted, (zero,) * MOMENTS, unroll=2))
    coef_load.wait()

    c_here = coef_in[place]
    nu = entries(total(0, groups), MOMENTS)
    factor = basis_steps(nu, c_here)
    for i in range(3):
        factors[place, i] = jnp.broadcast_to(factor[i], factors.shape[2:])

    late = pl.ds(EARLY, ny - EARLY)

    def combined(k, of_rows):
        j = low + k
        return field[j, of_rows] + (
            factor[0] * v0[j, of_rows]
            + (factor[1] * v1[j, of_rows] + factor[2] * v2[j, of_rows])
        )

    def update(k, _):
        u_send[k] = combined(k, late)
        return _

    lax.fori_loop(0, RING, update, 0, unroll=2)
    for chip, c in partners:
        issue(
            factors.at[place],
            factors.at[place],
            FACTORS,
            recv_sem.at[FACTORS],
            in_ring(chip, c),
        )
    for chip, c in outside + [partner]:
        number = 2 * chip + c
        issue(
            u_send.at[number],
            u_home.at[place, late],
            LATE_ROWS,
            recv_sem.at[LATE_ROWS],
            in_ring(chip, c),
        )
    early = pl.ds(0, EARLY)
    u_home[place, late] = u_send[place]
    u_home[place, early] = combined(place, early)

    g = entries(total(1, groups), MOMENTS)
    own = (
        factor[0] * factor[0] * g[0]
        + factor[1] * factor[1] * g[3]
        + factor[2] * factor[2] * g[5]
        + 2.0
        * (
            factor[0] * factor[1] * g[1]
            + factor[0] * factor[2] * g[2]
            + factor[1] * factor[2] * g[4]
        )
    )
    row = jnp.broadcast_to(own, (1, 128))
    own_rows[2] = row
    rows[2, place] = row
    for p in partners:
        remote(
            own_rows.at[2], rows.at[2, place], row_sent.at[2], row_recv.at[2], in_ring(*p)
        ).start()

    all_copies(EARLY_ROWS).wait_recv()
    all_copies(FACTORS).wait_recv()
    for chip, c in partners:
        s = 2 * chip + c
        u_home[s, early] = b_send[s, early] + (
            factors[s, 0] * v_home[s, 0]
            + (factors[s, 1] * v_home[s, 1] + factors[s, 2] * v_home[s, 2])
        )
    rms_out[...] = jnp.sqrt(total(2, RING)[0:1, 0:1] / cells)
    all_copies(LATE_ROWS).wait_recv()
    for kind in everything:
        all_copies(kind).wait_send()
    others(0, groups).wait_send()
    others(1, groups).wait_send()
    others(2, RING).wait_send()


def deliver(u, rms, u_out, rms_out, sems):
    copies = (
        pltpu.make_async_copy(u, u_out, sems.at[0]),
        pltpu.make_async_copy(rms, rms_out, sems.at[1]),
    )
    for copy in copies:
        copy.start()
    for copy in copies:
        copy.wait()


def shards(state, explicit_rhs, implicit_rhs, implicit_coef):
    species, _, ny, nx = state.shape
    sizes = (lax.axis_size(AXES[0]), lax.axis_size(AXES[1]))
    groups = sizes[0] * sizes[1]
    cells = species * ny * nx * groups * RING
    depth = RING + 2 * HALO
    f32 = jnp.float32
    hbm, vmem = (pl.BlockSpec(memory_space=m) for m in (pltpu.HBM, pltpu.VMEM))
    dma = pltpu.SemaphoreType.DMA
    u, rms = pl.pallas_call(
        functools.partial(kernel, sizes, cells),
        out_shape=(
            jax.ShapeDtypeStruct((species, ny, nx), f32),
            jax.ShapeDtypeStruct((1, 1), f32),
        ),
        in_specs=[hbm] * 4,
        out_specs=(vmem, vmem),
        scratch_shapes=[
            pltpu.VMEM((RING, ny, nx), f32),
            pltpu.VMEM((2, RING, ny, nx), f32),
            pltpu.VMEM((2, RING, ny, nx), f32),
            pltpu.SMEM((species,), f32),
            pltpu.VMEM((RING, ny, nx), f32),
            pltpu.VMEM((RING, ny, nx), f32),
            pltpu.VMEM((depth, ny, nx), f32),
            pltpu.VMEM((RING, ny, nx), f32),
            pltpu.VMEM((depth, ny, nx), f32),
            pltpu.VMEM((depth, ny, nx), f32),
            pltpu.VMEM((depth, ny, nx), f32),
            pltpu.VMEM((RING, 3, EARLY, nx), f32),
            pltpu.VMEM((RING, ny - EARLY, nx), f32),
            pltpu.VMEM((3, max(groups, RING), 1, 128), f32),
            pltpu.VMEM((3, 1, 128), f32),
            pltpu.VMEM((RING, 3, 1, nx), f32),
            dma((5,)),
            dma((RING,)),
            dma((2,)),
            dma((6,)),
            dma((6,)),
            dma((3,)),
            dma((3,)),
            pltpu.SemaphoreType.REGULAR((3,)),
        ],
        compiler_params=pltpu.CompilerParams(
            collective_id=0, has_side_effects=True, vmem_limit_bytes=24 * 2**20
        ),
        name="section",
    )(
        *(
            pltpu.with_memory_space_constraint(a, pltpu.HBM)
            for a in (state, explicit_rhs, implicit_rhs, implicit_coef)
        )
    )
    u, rms = pl.pallas_call(
        deliver,
        out_shape=(jax.ShapeDtypeStruct(u.shape, f32), jax.ShapeDtypeStruct((1, 1), f32)),
        in_specs=[vmem, vmem],
        out_specs=(hbm, hbm),
        scratch_shapes=[dma((2,))],
        compiler_params=pltpu.CompilerParams(vmem_limit_bytes=2**20),
        name="deliver",
    )(u, rms)
    return u.reshape(state.shape), rms[0, 0]


def solution(mesh):
    torus = Mesh(mesh.devices.reshape(-1, 8, 4, 2), AXES)
    placed = (
        P(None, AXES, None, None),
        P(None, None, AXES, None, None),
        P(None, None, AXES, None, None),
        P(),
    )
    return jax.shard_map(
        shards,
        mesh=torus,
        in_specs=placed,
        out_specs=(P(None, AXES, None, None), P()),
        check_vma=False,
    )
```

```python
import functools

import jax
import jax.numpy as jnp
from jax import lax
from jax.experimental import pallas as pl
from jax.experimental.pallas import tpu as pltpu
from jax.sharding import Mesh
from jax.sharding import PartitionSpec as P

AXES = ("gz_0", "gz_1", "gz_2", "gz_3")
MESH = pl.DeviceIdType.MESH

explicit_weights = (5535828885825.0 / 10492691773637.0, 788022342437.0 / 10882634858940.0)
implicit_weights = (2746238789719.0 / 10658868560708.0, -640167445237.0 / 6845629431997.0)

HALO = 4
RING = 8
MOMENTS = 6
SHIFT = 8.0
EARLY = 16


def remote(src, dst, send, recv, device):
    return pltpu.make_async_remote_copy(
        src_ref=src,
        dst_ref=dst,
        send_sem=send,
        recv_sem=recv,
        device_id=device,
        device_id_type=MESH,
    )


def laplace(below, here, above, shift=0.0):
    ny, nx = here.shape
    row = lax.broadcasted_iota(jnp.int32, here.shape, 0)
    lane = lax.broadcasted_iota(jnp.int32, here.shape, 1)
    beside = below + above
    beside = beside + jnp.where(row == ny - 1, 0.0, pltpu.roll(here, ny - 1, 0))
    beside = beside + jnp.where(row == 0, 0.0, pltpu.roll(here, 1, 0))
    beside = beside + jnp.where(lane == nx - 1, 0.0, pltpu.roll(here, nx - 1, 1))
    beside = beside + jnp.where(lane == 0, 0.0, pltpu.roll(here, 1, 1))
    return (6.0 - shift) * here - beside


def folded(value):
    total = value[0:8]
    for at in range(8, value.shape[0], 8):
        total = total + value[at : at + 8]
    return total


def row_of(sums):
    row = lax.broadcasted_iota(jnp.int32, (8, 128), 0)
    lane = lax.broadcasted_iota(jnp.int32, (8, 128), 1)
    stacked = jnp.zeros((8, 128), jnp.float32)
    for k, value in enumerate(sums):
        halves = sum(value[:, at : at + 128] for at in range(0, value.shape[1], 128))
        stacked = jnp.where(row == k, jnp.sum(halves, axis=0, keepdims=True), stacked)
    each = jnp.where(row == lane, jnp.sum(stacked, axis=1, keepdims=True), 0.0)
    return jnp.sum(each, axis=0, keepdims=True)


def entries(row, count):
    lane = lax.broadcasted_iota(jnp.int32, (1, 128), 1)
    return [
        jnp.sum(jnp.where(lane == k, row, 0.0), axis=1, keepdims=True) for k in range(count)
    ]


def basis_steps(nu, c):
    diagonal = 1.0 + SHIFT * c

    def gram(p, shift):
        total = None
        for i, a in enumerate(p):
            for j, b in enumerate(p):
                term = a * b * nu[i + j + shift]
                total = term if total is None else total + term
        return total

    def step(norm, along):
        energy = jnp.maximum(diagonal * gram(along, 0) + c * gram(along, 1), norm)
        return jnp.where(norm > 0.0, norm / energy, 0.0)

    norm = nu[0]
    first = norm / (diagonal * nu[0] + c * nu[1])
    residual = (1.0 - first * diagonal, -first * c)
    norm_next = jnp.maximum(gram(residual, 0), 0.0)
    ratio = norm_next / norm
    along = (residual[0] + ratio, residual[1])
    second = step(norm_next, along)
    norm = norm_next
    image = (diagonal * along[0], diagonal * along[1] + c * along[0], c * along[1])
    residual = (
        residual[0] - second * image[0],
        residual[1] - second * image[1],
        -second * image[2],
    )
    norm_next = jnp.maximum(gram(residual, 0), 0.0)
    ratio = jnp.where(norm > 0.0, norm_next / norm, 0.0)
    last = (residual[0] + ratio * along[0], residual[1] + ratio * along[1], residual[2])
    third = step(norm_next, last)
    return (
        -c * (first + second * along[0] + third * last[0]),
        -c * (second * along[1] + third * last[1]),
        -c * (third * last[2]),
    )


def kernel(
    sizes,
    cells,
    state,
    explicit,
    implicit,
    coef,
    u_home,
    rms_out,
    state_in,
    explicit_in,
    implicit_in,
    coef_in,
    b_send,
    d_send,
    field,
    weight,
    v0,
    v1,
    v2,
    v_home,
    u_send,
    rows,
    own_rows,
    factors,
    in_sem,
    b_recv,
    halo_recv,
    sent_sem,
    recv_sem,
    row_sent,
    row_recv,
    wave_sem,
):
    count_y, count_z = sizes
    groups = count_y * count_z
    ny = field.shape[1]
    y, z, x, core = (lax.axis_index(a) for a in AXES)
    place = 2 * x + core
    group = y * count_z + z
    right, left, across = lax.rem(x + 1, 4), lax.rem(x + 3, 4), lax.rem(x + 2, 4)

    flip = x // 2

    def in_ring(chip, c):
        return (y, z, chip, c)

    def layer(number, chip):
        turned = chip // 2
        return turned * (RING - 1) + (1 - 2 * turned) * number

    def at_group(step):
        of_group = lax.rem(group + step + groups, groups)
        return (of_group // count_z, lax.rem(of_group, count_z), x, core)

    def away(step_y, step_z):
        return (lax.rem(y + step_y, count_y), lax.rem(z + step_z + count_z, count_z), x, core)

    partner = (x, 1 - core)
    outside = [(chip, c) for c in (core, 1 - core) for chip in (across, right, left)]
    partners = [partner] + outside

    barrier = pltpu.get_barrier_semaphore()
    beside = [away(0, 1), away(0, -1), away(1, 0), away(count_y - 1, 0)]
    near = [in_ring(*p) for p in partners] + beside
    for device in near:
        pl.semaphore_signal(barrier, inc=1, device_id=device, device_id_type=MESH)

    for k, chip in enumerate((across, right, left, x)):
        pair = pl.ds(2 * chip, 2)
        for source, target in (
            (state.at[pair, 0], state_in.at[pair]),
            (explicit.at[:, pair, 0], explicit_in.at[:, pair]),
            (implicit.at[:, pair, 0], implicit_in.at[:, pair]),
        ):
            pltpu.make_async_copy(source, target, in_sem.at[k]).start()
    coef_load = pltpu.make_async_copy(coef, coef_in, in_sem.at[4])
    coef_load.start()

    def section_in(k, chip):
        ten = field.at[pl.ds(0, 10)]
        pltpu.make_async_copy(ten, ten, in_sem.at[k]).wait()
        for s in (2 * chip, 2 * chip + 1):
            b = (
                state_in[s]
                + explicit_weights[0] * explicit_in[0, s]
                + explicit_weights[1] * explicit_in[1, s]
            )
            b_send[s] = b + (
                implicit_weights[0] * implicit_in[0, s]
                + implicit_weights[1] * implicit_in[1, s]
            )

    BLOCK, HALO_BLOCK, WEIGHT, EARLY_ROWS, FACTORS, LATE_ROWS = range(6)

    def issue(source, target, kind, recv, device):
        remote(source, target, sent_sem.at[kind], recv, device).start()

    def some_copies(of, kind, recv):
        return remote(of, of, sent_sem.at[kind], recv, in_ring(right, core))

    def send_b(chip, c):
        issue(
            b_send.at[2 * chip + c],
            field.at[HALO + layer(place, chip)],
            BLOCK,
            b_recv.at[place],
            in_ring(chip, c),
        )

    def pass_on(number):
        origin = layer(number, x)
        half = origin // HALO

        @pl.when(origin != HALO)
        def _():
            issue(
                field.at[HALO + origin],
                field.at[lax.rem(origin + HALO + RING, HALO + RING + HALO)],
                HALO_BLOCK,
                halo_recv.at[1 - half],
                at_group((2 * half - 1) * (1 - 2 * flip)),
            )

    def b_arrived(chip, c):
        number = 2 * chip + c
        some_copies(field.at[HALO + layer(number, x)], BLOCK, b_recv.at[number]).wait_recv()
        return number

    section_in(0, across)
    pl.semaphore_wait(barrier, len(near))
    send_b(across, core)
    section_in(1, right)
    send_b(right, core)
    section_in(2, left)
    send_b(left, core)
    send_b(across, 1 - core)
    section_in(3, x)
    field[HALO + layer(place, x)] = b_send[place]
    send_b(*partner)
    send_b(right, 1 - core)
    send_b(left, 1 - core)

    waves = [beside, [away(0, k) for k in (1, -1, 2, -2)], [away(0, 2), away(0, -2)]]

    def wave(k):
        for device in waves[k]:
            pl.semaphore_signal(
                wave_sem.at[k], inc=1, device_id=device, device_id_type=MESH
            )

    def after_wave(k):
        pl.semaphore_wait(wave_sem.at[k], len(waves[k]))

    wave(0)

    def weigh(s, _):
        d = 1.0 / (1.0 + 0.1 * jnp.abs(state_in[s]))
        d_send[s] = d * d
        return _

    lax.fori_loop(0, RING, weigh, 0, unroll=2)
    weight[layer(place, x)] = d_send[place]
    for chip, c in partners:
        number = 2 * chip + c
        issue(
            d_send.at[number],
            weight.at[layer(place, chip)],
            WEIGHT,
            recv_sem.at[WEIGHT],
            in_ring(chip, c),
        )
    after_wave(0)
    wave(1)
    pass_on(place)
    pass_on(b_arrived(*partner))
    for p in (
        (across, core),
        (right, core),
        (left, core),
        (across, 1 - core),
        (right, 1 - core),
        (left, 1 - core),
    ):
        pass_on(b_arrived(*p))
    after_wave(1)
    wave(2)

    last = 2 * HALO + RING
    low, high = HALO, HALO + RING

    def planes(source, target, shift, start, stop):
        def body(j, _):
            target[j] = laplace(source[j - 1], source[j], source[j + 1], shift)
            return _

        lax.fori_loop(start, stop, body, 0, unroll=True)

    planes(field, v0, 0.0, low + 1, high - 1)
    planes(v0, v1, SHIFT, low + 2, high - 2)
    planes(v1, v2, SHIFT, low + 3, high - 3)
    zero = jnp.zeros((8, field.shape[-1]), jnp.float32)

    def moments(j, sums):
        a, b, e = v0[j], v1[j], v2[j]
        image = laplace(v2[j + 1], e, v2[j + 1], SHIFT)
        products = (a * a, a * b, b * b, b * e, e * e, e * image)
        return tuple(total + folded(product) for total, product in zip(sums, products))

    sums = (zero,) * MOMENTS
    middle = low + RING // 2
    for side, start, stop in (
        (0, lambda d: d + 1, lambda d: low + d),
        (1, lambda d: high - d, lambda d: last - d),
    ):
        blocks = field.at[pl.ds(1, 3) if side == 0 else pl.ds(high, HALO)]
        some_copies(blocks, HALO_BLOCK, halo_recv.at[side]).wait_recv()
        planes(field, v0, 0.0, start(1), stop(1))
        planes(v0, v1, SHIFT, start(2), stop(2))
        planes(v1, v2, SHIFT, start(3), stop(3))
        if side == 0:
            sums = lax.fori_loop(low, middle, moments, sums, unroll=2)

    for chip, c in outside + [partner]:
        number = 2 * chip + c
        for i, v in enumerate((v0, v1, v2)):
            issue(
                v.at[low + layer(number, x), pl.ds(0, EARLY)],
                v_home.at[place, i],
                EARLY_ROWS,
                recv_sem.at[EARLY_ROWS],
                in_ring(chip, c),
            )

    sums = lax.fori_loop(middle, high, moments, sums, unroll=2)

    far = sorted(
        ((dy, dz) for dy in range(count_y) for dz in range(count_z) if (dy, dz) != (0, 0)),
        key=lambda d: -min(d[0], count_y - d[0]) - min(d[1], count_z - d[1]),
    )

    def publish(phase, values):
        row = row_of(values)
        own_rows[phase] = row
        rows[phase, group] = row
        for step in far:
            remote(
                own_rows.at[phase],
                rows.at[phase, group],
                row_sent.at[phase],
                row_recv.at[phase],
                away(*step),
            ).start()

    def others(phase, count):
        some = rows.at[phase, pl.ds(0, count - 1)]
        return remote(
            some, some, row_sent.at[phase], row_recv.at[phase], in_ring(right, core)
        )

    def total(phase, count):
        others(phase, count).wait_recv()
        parts = [rows[phase, k] for k in range(count)]
        while len(parts) > 1:
            parts = [a + b for a, b in zip(parts[::2], parts[1::2])]
        return parts[0]

    after_wave(2)
    publish(0, sums)

    seven = pl.ds(0, RING - 1)
    everything = {
        BLOCK: b_send.at[seven],
        HALO_BLOCK: field.at[seven],
        WEIGHT: weight.at[seven],
        EARLY_ROWS: v_home.at[seven],
        FACTORS: factors.at[seven],
        LATE_ROWS: u_send.at[seven],
    }

    def all_copies(kind):
        return some_copies(everything[kind], kind, recv_sem.at[kind])

    all_copies(WEIGHT).wait_recv()

    def weighted(j, sums):
        d = weight[j - low]
        a, b, e = v0[j], v1[j], v2[j]
        da, db, de = d * a, d * b, d * e
        products = (da * a, da * b, da * e, db * b, db * e, de * e)
        return tuple(total + folded(product) for total, product in zip(sums, products))

    publish(1, lax.fori_loop(low, high, weighted, (zero,) * MOMENTS, unroll=2))
    coef_load.wait()

    c_here = coef_in[place]
    nu = entries(total(0, groups), MOMENTS)
    factor = basis_steps(nu, c_here)
    for i in range(3):
        factors[place, i] = jnp.broadcast_to(factor[i], factors.shape[2:])

    late = pl.ds(EARLY, ny - EARLY)

    def combined(k, of_rows):
        j = low + k
        return field[j, of_rows] + (
            factor[0] * v0[j, of_rows]
            + (factor[1] * v1[j, of_rows] + factor[2] * v2[j, of_rows])
        )

    def update(k, _):
        u_send[k] = combined(k, late)
        return _

    lax.fori_loop(0, RING, update, 0, unroll=2)
    for chip, c in partners:
        issue(
            factors.at[place],
            factors.at[place],
            FACTORS,
            recv_sem.at[FACTORS],
            in_ring(chip, c),
        )
    for chip, c in outside + [partner]:
        number = 2 * chip + c
        issue(
            u_send.at[layer(number, x)],
            u_home.at[place, late],
            LATE_ROWS,
            recv_sem.at[LATE_ROWS],
            in_ring(chip, c),
        )
    early = pl.ds(0, EARLY)
    mine = layer(place, x)
    u_home[place, late] = u_send[mine]
    u_home[place, early] = combined(mine, early)

    g = entries(total(1, groups), MOMENTS)
    own = (
        factor[0] * factor[0] * g[0]
        + factor[1] * factor[1] * g[3]
        + factor[2] * factor[2] * g[5]
        + 2.0
        * (
            factor[0] * factor[1] * g[1]
            + factor[0] * factor[2] * g[2]
            + factor[1] * factor[2] * g[4]
        )
    )
    row = jnp.broadcast_to(own, (1, 128))
    own_rows[2] = row
    rows[2, place] = row
    for p in partners:
        remote(
            own_rows.at[2], rows.at[2, place], row_sent.at[2], row_recv.at[2], in_ring(*p)
        ).start()

    all_copies(EARLY_ROWS).wait_recv()
    all_copies(FACTORS).wait_recv()
    for chip, c in partners:
        s = 2 * chip + c
        u_home[s, early] = b_send[s, early] + (
            factors[s, 0] * v_home[s, 0]
            + (factors[s, 1] * v_home[s, 1] + factors[s, 2] * v_home[s, 2])
        )
    rms_out[...] = jnp.broadcast_to(jnp.sqrt(total(2, RING) / cells), rms_out.shape)
    all_copies(LATE_ROWS).wait_recv()
    for kind in everything:
        all_copies(kind).wait_send()
    others(0, groups).wait_send()
    others(1, groups).wait_send()
    others(2, RING).wait_send()


def deliver(u, rms, u_out, rms_out, rms_row, sems):
    per = u.shape[0] // 1
    copies = [
        pltpu.make_async_copy(u.at[pl.ds(k * per, per)], u_out.at[pl.ds(k * per, per)], sems.at[k])
        for k in range(1)
    ]
    copies.append(pltpu.make_async_copy(rms_row, rms_out, sems.at[1]))
    for copy in copies[:-1]:
        copy.start()
    rms_row[...] = rms[0:1, 0:1]
    copies[-1].start()
    for copy in copies:
        copy.wait()


def shards(state, explicit_rhs, implicit_rhs, implicit_coef):
    species, _, ny, nx = state.shape
    sizes = (lax.axis_size(AXES[0]), lax.axis_size(AXES[1]))
    groups = sizes[0] * sizes[1]
    cells = species * ny * nx * groups * RING
    depth = RING + 2 * HALO
    f32 = jnp.float32
    hbm, vmem = (pl.BlockSpec(memory_space=m) for m in (pltpu.HBM, pltpu.VMEM))
    dma = pltpu.SemaphoreType.DMA
    u, rms = pl.pallas_call(
        functools.partial(kernel, sizes, cells),
        out_shape=(
            jax.ShapeDtypeStruct((species, ny, nx), f32),
            jax.ShapeDtypeStruct((8, 128), f32),
        ),
        in_specs=[hbm] * 4,
        out_specs=(vmem, vmem),
        scratch_shapes=[
            pltpu.VMEM((RING, ny, nx), f32),
            pltpu.VMEM((2, RING, ny, nx), f32),
            pltpu.VMEM((2, RING, ny, nx), f32),
            pltpu.SMEM((species,), f32),
            pltpu.VMEM((RING, ny, nx), f32),
            pltpu.VMEM((RING, ny, nx), f32),
            pltpu.VMEM((depth, ny, nx), f32),
            pltpu.VMEM((RING, ny, nx), f32),
            pltpu.VMEM((depth, ny, nx), f32),
            pltpu.VMEM((depth, ny, nx), f32),
            pltpu.VMEM((depth, ny, nx), f32),
            pltpu.VMEM((RING, 3, EARLY, nx), f32),
            pltpu.VMEM((RING, ny - EARLY, nx), f32),
            pltpu.VMEM((3, max(groups, RING), 1, 128), f32),
            pltpu.VMEM((3, 1, 128), f32),
            pltpu.VMEM((RING, 3, 1, nx), f32),
            dma((5,)),
            dma((RING,)),
            dma((2,)),
            dma((6,)),
            dma((6,)),
            dma((3,)),
            dma((3,)),
            pltpu.SemaphoreType.REGULAR((3,)),
        ],
        compiler_params=pltpu.CompilerParams(
            collective_id=0, has_side_effects=True, vmem_limit_bytes=24 * 2**20
        ),
        name="section",
    )(
        *(
            pltpu.with_memory_space_constraint(a, pltpu.HBM)
            for a in (state, explicit_rhs, implicit_rhs, implicit_coef)
        )
    )
    u, rms = pl.pallas_call(
        deliver,
        out_shape=(jax.ShapeDtypeStruct(u.shape, f32), jax.ShapeDtypeStruct((1, 1), f32)),
        in_specs=[vmem, vmem],
        out_specs=(hbm, hbm),
        scratch_shapes=[pltpu.VMEM((1, 1), f32), dma((2,))],
        compiler_params=pltpu.CompilerParams(vmem_limit_bytes=2**20),
        name="deliver",
    )(u, rms)
    return u.reshape(state.shape), rms[0, 0]


def solution(mesh):
    torus = Mesh(mesh.devices.reshape(-1, 8, 4, 2), AXES)
    placed = (
        P(None, AXES, None, None),
        P(None, None, AXES, None, None),
        P(None, None, AXES, None, None),
        P(),
    )
    return jax.shard_map(
        shards,
        mesh=torus,
        in_specs=placed,
        out_specs=(P(None, AXES, None, None), P()),
        check_vma=False,
    )
```

```python
import functools

import jax
import jax.numpy as jnp
from jax import lax
from jax.experimental import pallas as pl
from jax.experimental.pallas import tpu as pltpu
from jax.sharding import Mesh
from jax.sharding import PartitionSpec as P

AXES = ("gz_0", "gz_1", "gz_2", "gz_3")
MESH = pl.DeviceIdType.MESH

explicit_weights = (5535828885825.0 / 10492691773637.0, 788022342437.0 / 10882634858940.0)
implicit_weights = (2746238789719.0 / 10658868560708.0, -640167445237.0 / 6845629431997.0)

HALO = 4
RING = 8
MOMENTS = 6
SHIFT = 8.0
EARLY = 16


def remote(src, dst, send, recv, device):
    return pltpu.make_async_remote_copy(
        src_ref=src,
        dst_ref=dst,
        send_sem=send,
        recv_sem=recv,
        device_id=device,
        device_id_type=MESH,
    )


def laplace(below, here, above, shift=0.0):
    ny, nx = here.shape
    row = lax.broadcasted_iota(jnp.int32, here.shape, 0)
    lane = lax.broadcasted_iota(jnp.int32, here.shape, 1)
    beside = below + above
    beside = beside + jnp.where(row == ny - 1, 0.0, pltpu.roll(here, ny - 1, 0))
    beside = beside + jnp.where(row == 0, 0.0, pltpu.roll(here, 1, 0))
    beside = beside + jnp.where(lane == nx - 1, 0.0, pltpu.roll(here, nx - 1, 1))
    beside = beside + jnp.where(lane == 0, 0.0, pltpu.roll(here, 1, 1))
    return (6.0 - shift) * here - beside


def folded(value):
    total = value[0:8]
    for at in range(8, value.shape[0], 8):
        total = total + value[at : at + 8]
    return total


def row_of(sums):
    row = lax.broadcasted_iota(jnp.int32, (8, 128), 0)
    lane = lax.broadcasted_iota(jnp.int32, (8, 128), 1)
    stacked = jnp.zeros((8, 128), jnp.float32)
    for k, value in enumerate(sums):
        halves = sum(value[:, at : at + 128] for at in range(0, value.shape[1], 128))
        stacked = jnp.where(row == k, jnp.sum(halves, axis=0, keepdims=True), stacked)
    each = jnp.where(row == lane, jnp.sum(stacked, axis=1, keepdims=True), 0.0)
    return jnp.sum(each, axis=0, keepdims=True)


def entries(row, count):
    lane = lax.broadcasted_iota(jnp.int32, (1, 128), 1)
    return [
        jnp.sum(jnp.where(lane == k, row, 0.0), axis=1, keepdims=True) for k in range(count)
    ]


def basis_steps(nu, c):
    diagonal = 1.0 + SHIFT * c

    def gram(p, shift):
        total = None
        for i, a in enumerate(p):
            for j, b in enumerate(p):
                term = a * b * nu[i + j + shift]
                total = term if total is None else total + term
        return total

    def step(norm, along):
        energy = jnp.maximum(diagonal * gram(along, 0) + c * gram(along, 1), norm)
        return jnp.where(norm > 0.0, norm / energy, 0.0)

    norm = nu[0]
    first = norm / (diagonal * nu[0] + c * nu[1])
    residual = (1.0 - first * diagonal, -first * c)
    norm_next = jnp.maximum(gram(residual, 0), 0.0)
    ratio = norm_next / norm
    along = (residual[0] + ratio, residual[1])
    second = step(norm_next, along)
    norm = norm_next
    image = (diagonal * along[0], diagonal * along[1] + c * along[0], c * along[1])
    residual = (
        residual[0] - second * image[0],
        residual[1] - second * image[1],
        -second * image[2],
    )
    norm_next = jnp.maximum(gram(residual, 0), 0.0)
    ratio = jnp.where(norm > 0.0, norm_next / norm, 0.0)
    last = (residual[0] + ratio * along[0], residual[1] + ratio * along[1], residual[2])
    third = step(norm_next, last)
    return (
        -c * (first + second * along[0] + third * last[0]),
        -c * (second * along[1] + third * last[1]),
        -c * (third * last[2]),
    )


def kernel(
    sizes,
    cells,
    state,
    explicit,
    implicit,
    coef,
    u_home,
    rms_out,
    state_in,
    explicit_in,
    implicit_in,
    coef_in,
    b_send,
    d_send,
    field,
    weight,
    v0,
    v1,
    v2,
    v_home,
    u_send,
    rows,
    own_rows,
    factors,
    in_sem,
    b_recv,
    halo_recv,
    sent_sem,
    recv_sem,
    row_sent,
    row_recv,
    wave_sem,
):
    count_y, count_z = sizes
    groups = count_y * count_z
    ny = field.shape[1]
    y, z, x, core = (lax.axis_index(a) for a in AXES)
    place = 2 * x + core
    group = y * count_z + z
    right, left, across = lax.rem(x + 1, 4), lax.rem(x + 3, 4), lax.rem(x + 2, 4)

    flip = x // 2

    def in_ring(chip, c):
        return (y, z, chip, c)

    def layer(number, chip):
        turned = chip // 2
        return turned * (RING - 1) + (1 - 2 * turned) * number

    def at_group(step):
        of_group = lax.rem(group + step + groups, groups)
        return (of_group // count_z, lax.rem(of_group, count_z), x, core)

    def away(step_y, step_z):
        return (lax.rem(y + step_y, count_y), lax.rem(z + step_z + count_z, count_z), x, core)

    partner = (x, 1 - core)
    outside = [(chip, c) for c in (core, 1 - core) for chip in (across, right, left)]
    partners = [partner] + outside

    barrier = pltpu.get_barrier_semaphore()
    beside = [away(0, 1), away(0, -1), away(1, 0), away(count_y - 1, 0)]
    near = [in_ring(*p) for p in partners] + beside
    for device in near:
        pl.semaphore_signal(barrier, inc=1, device_id=device, device_id_type=MESH)

    for k, chip in enumerate((across, right, left, x)):
        pair = pl.ds(2 * chip, 2)
        for source, target in (
            (state.at[pair, 0], state_in.at[pair]),
            (explicit.at[:, pair, 0], explicit_in.at[:, pair]),
            (implicit.at[:, pair, 0], implicit_in.at[:, pair]),
        ):
            pltpu.make_async_copy(source, target, in_sem.at[k]).start()
    coef_load = pltpu.make_async_copy(coef, coef_in, in_sem.at[4])
    coef_load.start()

    def section_in(k, chip):
        ten = field.at[pl.ds(0, 10)]
        pltpu.make_async_copy(ten, ten, in_sem.at[k]).wait()
        for s in (2 * chip, 2 * chip + 1):
            b = (
                state_in[s]
                + explicit_weights[0] * explicit_in[0, s]
                + explicit_weights[1] * explicit_in[1, s]
            )
            b_send[s] = b + (
                implicit_weights[0] * implicit_in[0, s]
                + implicit_weights[1] * implicit_in[1, s]
            )

    BLOCK, HALO_BLOCK, WEIGHT, EARLY_ROWS, FACTORS, LATE_ROWS = range(6)

    def issue(source, target, kind, recv, device):
        remote(source, target, sent_sem.at[kind], recv, device).start()

    def some_copies(of, kind, recv):
        return remote(of, of, sent_sem.at[kind], recv, in_ring(right, core))

    def send_b(chip, c):
        issue(
            b_send.at[2 * chip + c],
            field.at[HALO + layer(place, chip)],
            BLOCK,
            b_recv.at[place],
            in_ring(chip, c),
        )

    def pass_on(number):
        origin = layer(number, x)
        half = origin // HALO

        @pl.when(origin != HALO)
        def _():
            issue(
                field.at[HALO + origin],
                field.at[lax.rem(origin + HALO + RING, HALO + RING + HALO)],
                HALO_BLOCK,
                halo_recv.at[1 - half],
                at_group((2 * half - 1) * (1 - 2 * flip)),
            )

    def b_arrived(chip, c):
        number = 2 * chip + c
        some_copies(field.at[HALO + layer(number, x)], BLOCK, b_recv.at[number]).wait_recv()
        return number

    section_in(0, across)
    pl.semaphore_wait(barrier, len(near))
    send_b(across, core)
    section_in(1, right)
    send_b(right, core)
    section_in(2, left)
    send_b(left, core)
    send_b(across, 1 - core)
    section_in(3, x)
    field[HALO + layer(place, x)] = b_send[place]
    send_b(*partner)
    send_b(right, 1 - core)
    send_b(left, 1 - core)

    waves = [beside, [away(0, k) for k in (1, -1, 2, -2)], [away(0, 2), away(0, -2)]]

    def wave(k):
        for device in waves[k]:
            pl.semaphore_signal(
                wave_sem.at[k], inc=1, device_id=device, device_id_type=MESH
            )

    def after_wave(k):
        pl.semaphore_wait(wave_sem.at[k], len(waves[k]))

    wave(0)

    def weigh(s, _):
        d = 1.0 / (1.0 + 0.1 * jnp.abs(state_in[s]))
        d_send[s] = d * d
        return _

    lax.fori_loop(0, RING, weigh, 0, unroll=2)
    weight[layer(place, x)] = d_send[place]
    after_wave(0)
    wave(1)
    pass_on(place)
    pass_on(b_arrived(*partner))
    for p in ((across, core), (right, core), (left, core), (across, 1 - core)):
        pass_on(b_arrived(*p))
    for chip, c in partners:
        number = 2 * chip + c
        issue(
            d_send.at[number],
            weight.at[layer(place, chip)],
            WEIGHT,
            recv_sem.at[WEIGHT],
            in_ring(chip, c),
        )
    for p in ((right, 1 - core), (left, 1 - core)):
        pass_on(b_arrived(*p))
    after_wave(1)
    wave(2)

    last = 2 * HALO + RING
    low, high = HALO, HALO + RING

    def planes(source, target, shift, start, stop):
        def body(j, _):
            target[j] = laplace(source[j - 1], source[j], source[j + 1], shift)
            return _

        lax.fori_loop(start, stop, body, 0, unroll=True)

    planes(field, v0, 0.0, low + 1, high - 1)
    planes(v0, v1, SHIFT, low + 2, high - 2)
    planes(v1, v2, SHIFT, low + 3, high - 3)
    zero = jnp.zeros((8, field.shape[-1]), jnp.float32)

    def moments(j, sums):
        a, b, e = v0[j], v1[j], v2[j]
        image = laplace(v2[j + 1], e, v2[j + 1], SHIFT)
        products = (a * a, a * b, b * b, b * e, e * e, e * image)
        return tuple(total + folded(product) for total, product in zip(sums, products))

    sums = (zero,) * MOMENTS
    middle = low + RING // 2
    for side, start, stop in (
        (1, lambda d: high - d, lambda d: last - d),
        (0, lambda d: d + 1, lambda d: low + d),
    ):
        blocks = field.at[pl.ds(1, 3) if side == 0 else pl.ds(high, HALO)]
        some_copies(blocks, HALO_BLOCK, halo_recv.at[side]).wait_recv()
        planes(field, v0, 0.0, start(1), stop(1))
        planes(v0, v1, SHIFT, start(2), stop(2))
        planes(v1, v2, SHIFT, start(3), stop(3))
        if side == 1:
            sums = lax.fori_loop(middle, high, moments, sums, unroll=True)

    for chip, c in outside + [partner]:
        number = 2 * chip + c
        for i, v in enumerate((v0, v1, v2)):
            issue(
                v.at[low + layer(number, x), pl.ds(0, EARLY)],
                v_home.at[place, i],
                EARLY_ROWS,
                recv_sem.at[EARLY_ROWS],
                in_ring(chip, c),
            )

    sums = lax.fori_loop(low, middle, moments, sums, unroll=True)

    far = sorted(
        ((dy, dz) for dy in range(count_y) for dz in range(count_z) if (dy, dz) != (0, 0)),
        key=lambda d: -min(d[0], count_y - d[0]) - min(d[1], count_z - d[1]),
    )

    def publish(phase, values):
        row = row_of(values)
        own_rows[phase] = row
        rows[phase, group] = row
        for step in far:
            remote(
                own_rows.at[phase],
                rows.at[phase, group],
                row_sent.at[phase],
                row_recv.at[phase],
                away(*step),
            ).start()

    def others(phase, count):
        some = rows.at[phase, pl.ds(0, count - 1)]
        return remote(
            some, some, row_sent.at[phase], row_recv.at[phase], in_ring(right, core)
        )

    def total(phase, count):
        others(phase, count).wait_recv()
        parts = [rows[phase, k] for k in range(count)]
        while len(parts) > 1:
            parts = [a + b for a, b in zip(parts[::2], parts[1::2])]
        return parts[0]

    after_wave(2)
    publish(0, sums)

    seven = pl.ds(0, RING - 1)
    everything = {
        BLOCK: b_send.at[seven],
        HALO_BLOCK: field.at[seven],
        WEIGHT: weight.at[seven],
        EARLY_ROWS: v_home.at[seven],
        FACTORS: factors.at[seven],
        LATE_ROWS: u_send.at[seven],
    }

    def all_copies(kind):
        return some_copies(everything[kind], kind, recv_sem.at[kind])

    all_copies(WEIGHT).wait_recv()

    def weighted(j, sums):
        d = weight[j - low]
        a, b, e = v0[j], v1[j], v2[j]
        da, db, de = d * a, d * b, d * e
        products = (da * a, da * b, da * e, db * b, db * e, de * e)
        return tuple(total + folded(product) for total, product in zip(sums, products))

    publish(1, lax.fori_loop(low, high, weighted, (zero,) * MOMENTS, unroll=2))
    coef_load.wait()

    c_here = coef_in[place]
    nu = entries(total(0, groups), MOMENTS)
    factor = basis_steps(nu, c_here)
    for i in range(3):
        factors[place, i] = jnp.broadcast_to(factor[i], factors.shape[2:])

    late = pl.ds(EARLY, ny - EARLY)

    def combined(k, of_rows):
        j = low + k
        return field[j, of_rows] + (
            factor[0] * v0[j, of_rows]
            + (factor[1] * v1[j, of_rows] + factor[2] * v2[j, of_rows])
        )

    def update(k, _):
        u_send[k] = combined(k, late)
        return _

    lax.fori_loop(0, RING, update, 0, unroll=2)
    for chip, c in partners:
        issue(
            factors.at[place],
            factors.at[place],
            FACTORS,
            recv_sem.at[FACTORS],
            in_ring(chip, c),
        )
    def send_u(*devices):
        for chip, c in devices:
            issue(
                u_send.at[layer(2 * chip + c, x)],
                u_home.at[place, late],
                LATE_ROWS,
                recv_sem.at[LATE_ROWS],
                in_ring(chip, c),
            )

    send_u((across, core), (across, 1 - core))

    g = entries(total(1, groups), MOMENTS)
    own = (
        factor[0] * factor[0] * g[0]
        + factor[1] * factor[1] * g[3]
        + factor[2] * factor[2] * g[5]
        + 2.0
        * (
            factor[0] * factor[1] * g[1]
            + factor[0] * factor[2] * g[2]
            + factor[1] * factor[2] * g[4]
        )
    )
    row = jnp.broadcast_to(own, (1, 128))
    own_rows[2] = row
    rows[2, place] = row
    for p in partners:
        remote(
            own_rows.at[2], rows.at[2, place], row_sent.at[2], row_recv.at[2], in_ring(*p)
        ).start()

    send_u((right, core), (left, core), partner, (right, 1 - core), (left, 1 - core))
    early = pl.ds(0, EARLY)
    mine = layer(place, x)
    u_home[place, late] = u_send[mine]
    u_home[place, early] = combined(mine, early)


    all_copies(EARLY_ROWS).wait_recv()
    all_copies(FACTORS).wait_recv()
    for chip, c in partners:
        s = 2 * chip + c
        u_home[s, early] = b_send[s, early] + (
            factors[s, 0] * v_home[s, 0]
            + (factors[s, 1] * v_home[s, 1] + factors[s, 2] * v_home[s, 2])
        )
    rms_out[...] = jnp.broadcast_to(jnp.sqrt(total(2, RING) / cells), rms_out.shape)
    all_copies(LATE_ROWS).wait_recv()
    for kind in everything:
        all_copies(kind).wait_send()
    others(0, groups).wait_send()
    others(1, groups).wait_send()
    others(2, RING).wait_send()


def deliver(u, rms, u_out, rms_out, rms_row, sems):
    per = u.shape[0] // 1
    copies = [
        pltpu.make_async_copy(u.at[pl.ds(k * per, per)], u_out.at[pl.ds(k * per, per)], sems.at[k])
        for k in range(1)
    ]
    copies.append(pltpu.make_async_copy(rms_row, rms_out, sems.at[1]))
    for copy in copies[:-1]:
        copy.start()
    rms_row[...] = rms[0:1, 0:1]
    copies[-1].start()
    for copy in copies:
        copy.wait()


def shards(state, explicit_rhs, implicit_rhs, implicit_coef):
    species, _, ny, nx = state.shape
    sizes = (lax.axis_size(AXES[0]), lax.axis_size(AXES[1]))
    groups = sizes[0] * sizes[1]
    cells = species * ny * nx * groups * RING
    depth = RING + 2 * HALO
    f32 = jnp.float32
    hbm, vmem = (pl.BlockSpec(memory_space=m) for m in (pltpu.HBM, pltpu.VMEM))
    dma = pltpu.SemaphoreType.DMA
    u, rms = pl.pallas_call(
        functools.partial(kernel, sizes, cells),
        out_shape=(
            jax.ShapeDtypeStruct((species, ny, nx), f32),
            jax.ShapeDtypeStruct((8, 128), f32),
        ),
        in_specs=[hbm] * 4,
        out_specs=(vmem, vmem),
        scratch_shapes=[
            pltpu.VMEM((RING, ny, nx), f32),
            pltpu.VMEM((2, RING, ny, nx), f32),
            pltpu.VMEM((2, RING, ny, nx), f32),
            pltpu.SMEM((species,), f32),
            pltpu.VMEM((RING, ny, nx), f32),
            pltpu.VMEM((RING, ny, nx), f32),
            pltpu.VMEM((depth, ny, nx), f32),
            pltpu.VMEM((RING, ny, nx), f32),
            pltpu.VMEM((depth, ny, nx), f32),
            pltpu.VMEM((depth, ny, nx), f32),
            pltpu.VMEM((depth, ny, nx), f32),
            pltpu.VMEM((RING, 3, EARLY, nx), f32),
            pltpu.VMEM((RING, ny - EARLY, nx), f32),
            pltpu.VMEM((3, max(groups, RING), 1, 128), f32),
            pltpu.VMEM((3, 1, 128), f32),
            pltpu.VMEM((RING, 3, 1, nx), f32),
            dma((5,)),
            dma((RING,)),
            dma((2,)),
            dma((6,)),
            dma((6,)),
            dma((3,)),
            dma((3,)),
            pltpu.SemaphoreType.REGULAR((3,)),
        ],
        compiler_params=pltpu.CompilerParams(
            collective_id=0, has_side_effects=True, vmem_limit_bytes=24 * 2**20
        ),
        name="section",
    )(
        *(
            pltpu.with_memory_space_constraint(a, pltpu.HBM)
            for a in (state, explicit_rhs, implicit_rhs, implicit_coef)
        )
    )
    u, rms = pl.pallas_call(
        deliver,
        out_shape=(jax.ShapeDtypeStruct(u.shape, f32), jax.ShapeDtypeStruct((1, 1), f32)),
        in_specs=[vmem, vmem],
        out_specs=(hbm, hbm),
        scratch_shapes=[pltpu.VMEM((1, 1), f32), dma((2,))],
        compiler_params=pltpu.CompilerParams(vmem_limit_bytes=2**20),
        name="deliver",
    )(u, rms)
    return u.reshape(state.shape), rms[0, 0]


def solution(mesh):
    torus = Mesh(mesh.devices.reshape(-1, 8, 4, 2), AXES)
    placed = (
        P(None, AXES, None, None),
        P(None, None, AXES, None, None),
        P(None, None, AXES, None, None),
        P(),
    )
    return jax.shard_map(
        shards,
        mesh=torus,
        in_specs=placed,
        out_specs=(P(None, AXES, None, None), P()),
        check_vma=False,
    )
```

```python
import functools

import jax
import jax.numpy as jnp
from jax import lax
from jax.experimental import pallas as pl
from jax.experimental.pallas import tpu as pltpu
from jax.sharding import Mesh
from jax.sharding import PartitionSpec as P

AXES = ("gz_0", "gz_1", "gz_2", "gz_3")
MESH = pl.DeviceIdType.MESH

explicit_weights = (5535828885825.0 / 10492691773637.0, 788022342437.0 / 10882634858940.0)
implicit_weights = (2746238789719.0 / 10658868560708.0, -640167445237.0 / 6845629431997.0)

HALO = 4
RING = 8
MOMENTS = 6
SHIFT = 8.0
EARLY = 16


def remote(src, dst, send, recv, device):
    return pltpu.make_async_remote_copy(
        src_ref=src,
        dst_ref=dst,
        send_sem=send,
        recv_sem=recv,
        device_id=device,
        device_id_type=MESH,
    )


def laplace(below, here, above, shift=0.0):
    ny, nx = here.shape
    row = lax.broadcasted_iota(jnp.int32, here.shape, 0)
    lane = lax.broadcasted_iota(jnp.int32, here.shape, 1)
    beside = below + above
    beside = beside + jnp.where(row == ny - 1, 0.0, pltpu.roll(here, ny - 1, 0))
    beside = beside + jnp.where(row == 0, 0.0, pltpu.roll(here, 1, 0))
    beside = beside + jnp.where(lane == nx - 1, 0.0, pltpu.roll(here, nx - 1, 1))
    beside = beside + jnp.where(lane == 0, 0.0, pltpu.roll(here, 1, 1))
    return (6.0 - shift) * here - beside


def folded(value):
    total = value[0:8]
    for at in range(8, value.shape[0], 8):
        total = total + value[at : at + 8]
    return total


def row_of(sums):
    row = lax.broadcasted_iota(jnp.int32, (8, 128), 0)
    lane = lax.broadcasted_iota(jnp.int32, (8, 128), 1)
    stacked = jnp.zeros((8, 128), jnp.float32)
    for k, value in enumerate(sums):
        halves = sum(value[:, at : at + 128] for at in range(0, value.shape[1], 128))
        stacked = jnp.where(row == k, jnp.sum(halves, axis=0, keepdims=True), stacked)
    each = jnp.where(row == lane, jnp.sum(stacked, axis=1, keepdims=True), 0.0)
    return jnp.sum(each, axis=0, keepdims=True)


def entries(row, count):
    lane = lax.broadcasted_iota(jnp.int32, (1, 128), 1)
    return [
        jnp.sum(jnp.where(lane == k, row, 0.0), axis=1, keepdims=True) for k in range(count)
    ]


def basis_steps(nu, c):
    diagonal = 1.0 + SHIFT * c

    def gram(p, shift):
        total = None
        for i, a in enumerate(p):
            for j, b in enumerate(p):
                term = a * b * nu[i + j + shift]
                total = term if total is None else total + term
        return total

    def step(norm, along):
        energy = jnp.maximum(diagonal * gram(along, 0) + c * gram(along, 1), norm)
        return jnp.where(norm > 0.0, norm / energy, 0.0)

    norm = nu[0]
    first = norm / (diagonal * nu[0] + c * nu[1])
    residual = (1.0 - first * diagonal, -first * c)
    norm_next = jnp.maximum(gram(residual, 0), 0.0)
    ratio = norm_next / norm
    along = (residual[0] + ratio, residual[1])
    second = step(norm_next, along)
    norm = norm_next
    image = (diagonal * along[0], diagonal * along[1] + c * along[0], c * along[1])
    residual = (
        residual[0] - second * image[0],
        residual[1] - second * image[1],
        -second * image[2],
    )
    norm_next = jnp.maximum(gram(residual, 0), 0.0)
    ratio = jnp.where(norm > 0.0, norm_next / norm, 0.0)
    last = (residual[0] + ratio * along[0], residual[1] + ratio * along[1], residual[2])
    third = step(norm_next, last)
    return (
        -c * (first + second * along[0] + third * last[0]),
        -c * (second * along[1] + third * last[1]),
        -c * (third * last[2]),
    )


def kernel(
    sizes,
    cells,
    state,
    explicit,
    implicit,
    coef,
    u_home,
    rms_out,
    state_in,
    explicit_in,
    implicit_in,
    coef_in,
    b_send,
    d_send,
    field,
    weight,
    v0,
    v1,
    v2,
    v_home,
    u_send,
    rows,
    own_rows,
    factors,
    in_sem,
    b_recv,
    halo_recv,
    sent_sem,
    recv_sem,
    row_sent,
    row_recv,
    wave_sem,
):
    count_y, count_z = sizes
    groups = count_y * count_z
    ny = field.shape[1]
    y, z, x, core = (lax.axis_index(a) for a in AXES)
    place = 2 * x + core
    group = y * count_z + z
    right, left, across = lax.rem(x + 1, 4), lax.rem(x + 3, 4), lax.rem(x + 2, 4)

    flip = x // 2

    def in_ring(chip, c):
        return (y, z, chip, c)

    def layer(number, chip):
        turned = chip // 2
        return turned * (RING - 1) + (1 - 2 * turned) * number

    def at_group(step):
        of_group = lax.rem(group + step + groups, groups)
        return (of_group // count_z, lax.rem(of_group, count_z), x, core)

    def away(step_y, step_z):
        return (lax.rem(y + step_y, count_y), lax.rem(z + step_z + count_z, count_z), x, core)

    partner = (x, 1 - core)
    outside = [(chip, c) for c in (core, 1 - core) for chip in (across, right, left)]
    partners = [partner] + outside

    barrier = pltpu.get_barrier_semaphore()
    beside = [away(0, 1), away(0, -1), away(1, 0), away(count_y - 1, 0)]
    near = [in_ring(*p) for p in partners] + beside
    for device in near:
        pl.semaphore_signal(barrier, inc=1, device_id=device, device_id_type=MESH)

    for k, chip in enumerate((across, right, left, x)):
        pair = pl.ds(2 * chip, 2)
        for source, target in (
            (state.at[pair, 0], state_in.at[pair]),
            (explicit.at[:, pair, 0], explicit_in.at[:, pair]),
            (implicit.at[:, pair, 0], implicit_in.at[:, pair]),
        ):
            pltpu.make_async_copy(source, target, in_sem.at[k]).start()
    coef_load = pltpu.make_async_copy(coef, coef_in, in_sem.at[4])
    coef_load.start()

    def section_in(k, chip):
        ten = field.at[pl.ds(0, 10)]
        pltpu.make_async_copy(ten, ten, in_sem.at[k]).wait()
        for s in (2 * chip, 2 * chip + 1):
            b = (
                state_in[s]
                + explicit_weights[0] * explicit_in[0, s]
                + explicit_weights[1] * explicit_in[1, s]
            )
            b_send[s] = b + (
                implicit_weights[0] * implicit_in[0, s]
                + implicit_weights[1] * implicit_in[1, s]
            )

    BLOCK, HALO_BLOCK, WEIGHT, EARLY_ROWS, FACTORS, LATE_ROWS = range(6)

    def issue(source, target, kind, recv, device):
        remote(source, target, sent_sem.at[kind], recv, device).start()

    def some_copies(of, kind, recv):
        return remote(of, of, sent_sem.at[kind], recv, in_ring(right, core))

    def send_b(chip, c):
        issue(
            b_send.at[2 * chip + c],
            field.at[HALO + layer(place, chip)],
            BLOCK,
            b_recv.at[place],
            in_ring(chip, c),
        )

    def pass_on(number):
        origin = layer(number, x)
        half = origin // HALO

        @pl.when(origin != HALO)
        def _():
            issue(
                field.at[HALO + origin],
                field.at[lax.rem(origin + HALO + RING, HALO + RING + HALO)],
                HALO_BLOCK,
                halo_recv.at[1 - half],
                at_group((2 * half - 1) * (1 - 2 * flip)),
            )

    def b_arrived(chip, c):
        number = 2 * chip + c
        some_copies(field.at[HALO + layer(number, x)], BLOCK, b_recv.at[number]).wait_recv()
        return number

    section_in(0, across)
    pl.semaphore_wait(barrier, len(near))
    send_b(across, core)
    section_in(1, right)
    send_b(right, core)
    section_in(2, left)
    send_b(left, core)
    send_b(across, 1 - core)
    section_in(3, x)
    field[HALO + layer(place, x)] = b_send[place]
    send_b(*partner)
    send_b(right, 1 - core)
    send_b(left, 1 - core)

    waves = [beside, [away(0, k) for k in (1, -1, 2, -2)], [away(0, 2), away(0, -2)]]

    def wave(k):
        for device in waves[k]:
            pl.semaphore_signal(
                wave_sem.at[k], inc=1, device_id=device, device_id_type=MESH
            )

    def after_wave(k):
        pl.semaphore_wait(wave_sem.at[k], len(waves[k]))

    wave(0)

    def weigh(s, _):
        d = 1.0 / (1.0 + 0.1 * jnp.abs(state_in[s]))
        d_send[s] = d * d
        return _

    lax.fori_loop(0, RING, weigh, 0, unroll=2)
    weight[layer(place, x)] = d_send[place]
    after_wave(0)
    wave(1)
    pass_on(place)
    pass_on(b_arrived(*partner))
    for p in ((across, core), (right, core), (left, core), (across, 1 - core)):
        pass_on(b_arrived(*p))
    for chip, c in partners:
        number = 2 * chip + c
        issue(
            d_send.at[number],
            weight.at[layer(place, chip)],
            WEIGHT,
            recv_sem.at[WEIGHT],
            in_ring(chip, c),
        )
    for p in ((right, 1 - core), (left, 1 - core)):
        pass_on(b_arrived(*p))
    after_wave(1)
    wave(2)

    last = 2 * HALO + RING
    low, high = HALO, HALO + RING

    def planes(source, target, shift, start, stop):
        def body(j, _):
            target[j] = laplace(source[j - 1], source[j], source[j + 1], shift)
            return _

        lax.fori_loop(start, stop, body, 0, unroll=True)

    planes(field, v0, 0.0, low + 1, high - 1)
    planes(v0, v1, SHIFT, low + 2, high - 2)
    planes(v1, v2, SHIFT, low + 3, high - 3)
    zero = jnp.zeros((8, field.shape[-1]), jnp.float32)

    def moments(j, sums):
        a, b, e = v0[j], v1[j], v2[j]
        image = laplace(v2[j + 1], e, v2[j + 1], SHIFT)
        products = (a * a, a * b, b * b, b * e, e * e, e * image)
        return tuple(total + folded(product) for total, product in zip(sums, products))

    sums = (zero,) * MOMENTS
    middle = low + RING // 2
    for side, start, stop in (
        (1, lambda d: high - d, lambda d: last - d),
        (0, lambda d: d + 1, lambda d: low + d),
    ):
        blocks = field.at[pl.ds(1, 3) if side == 0 else pl.ds(high, HALO)]
        some_copies(blocks, HALO_BLOCK, halo_recv.at[side]).wait_recv()
        planes(field, v0, 0.0, start(1), stop(1))
        planes(v0, v1, SHIFT, start(2), stop(2))
        planes(v1, v2, SHIFT, start(3), stop(3))
        if side == 1:
            sums = lax.fori_loop(middle, high, moments, sums, unroll=True)

    for chip, c in outside + [partner]:
        number = 2 * chip + c
        for i, v in enumerate((v0, v1, v2)):
            issue(
                v.at[low + layer(number, x), pl.ds(0, EARLY)],
                v_home.at[place, i],
                EARLY_ROWS,
                recv_sem.at[EARLY_ROWS],
                in_ring(chip, c),
            )

    sums = lax.fori_loop(low, middle, moments, sums, unroll=True)

    far = sorted(
        ((dy, dz) for dy in range(count_y) for dz in range(count_z) if (dy, dz) != (0, 0)),
        key=lambda d: -min(d[0], count_y - d[0]) - min(d[1], count_z - d[1]),
    )

    def publish(phase, values):
        row = row_of(values)
        own_rows[phase] = row
        rows[phase, group] = row
        for step in far:
            remote(
                own_rows.at[phase],
                rows.at[phase, group],
                row_sent.at[phase],
                row_recv.at[phase],
                away(*step),
            ).start()

    def others(phase, count):
        some = rows.at[phase, pl.ds(0, count - 1)]
        return remote(
            some, some, row_sent.at[phase], row_recv.at[phase], in_ring(right, core)
        )

    def total(phase, count):
        others(phase, count).wait_recv()
        parts = [rows[phase, k] for k in range(count)]
        while len(parts) > 1:
            parts = [a + b for a, b in zip(parts[::2], parts[1::2])]
        return parts[0]

    after_wave(2)
    publish(0, sums)

    seven = pl.ds(0, RING - 1)
    everything = {
        BLOCK: b_send.at[seven],
        HALO_BLOCK: field.at[seven],
        WEIGHT: weight.at[seven],
        EARLY_ROWS: v_home.at[seven],
        FACTORS: factors.at[seven],
        LATE_ROWS: u_send.at[seven],
    }

    def all_copies(kind):
        return some_copies(everything[kind], kind, recv_sem.at[kind])

    all_copies(WEIGHT).wait_recv()

    def weighted(j, sums):
        d = weight[j - low]
        a, b, e = v0[j], v1[j], v2[j]
        da, db, de = d * a, d * b, d * e
        products = (da * a, da * b, da * e, db * b, db * e, de * e)
        return tuple(total + folded(product) for total, product in zip(sums, products))

    publish(1, lax.fori_loop(low, high, weighted, (zero,) * MOMENTS, unroll=2))
    coef_load.wait()

    c_here = coef_in[place]
    nu = entries(total(0, groups), MOMENTS)
    factor = basis_steps(nu, c_here)
    for i in range(3):
        factors[place, i] = jnp.broadcast_to(factor[i], factors.shape[2:])

    late = pl.ds(EARLY, ny - EARLY)

    def combined(k, of_rows):
        j = low + k
        return field[j, of_rows] + (
            factor[0] * v0[j, of_rows]
            + (factor[1] * v1[j, of_rows] + factor[2] * v2[j, of_rows])
        )

    def update(k, _):
        u_send[k] = combined(k, late)
        return _

    lax.fori_loop(0, RING, update, 0, unroll=2)
    for chip, c in partners:
        issue(
            factors.at[place],
            factors.at[place],
            FACTORS,
            recv_sem.at[FACTORS],
            in_ring(chip, c),
        )
    def send_u(*devices):
        for chip, c in devices:
            issue(
                u_send.at[layer(2 * chip + c, x)],
                u_home.at[place, late],
                LATE_ROWS,
                recv_sem.at[LATE_ROWS],
                in_ring(chip, c),
            )

    send_u((across, core), (right, core), (left, core), (across, 1 - core))

    g = entries(total(1, groups), MOMENTS)
    own = (
        factor[0] * factor[0] * g[0]
        + factor[1] * factor[1] * g[3]
        + factor[2] * factor[2] * g[5]
        + 2.0
        * (
            factor[0] * factor[1] * g[1]
            + factor[0] * factor[2] * g[2]
            + factor[1] * factor[2] * g[4]
        )
    )
    row = jnp.broadcast_to(own, (1, 128))
    own_rows[2] = row
    rows[2, place] = row
    for p in partners:
        remote(
            own_rows.at[2], rows.at[2, place], row_sent.at[2], row_recv.at[2], in_ring(*p)
        ).start()

    send_u(partner, (right, 1 - core), (left, 1 - core))
    early = pl.ds(0, EARLY)
    mine = layer(place, x)
    u_home[place, late] = u_send[mine]
    u_home[place, early] = combined(mine, early)


    all_copies(EARLY_ROWS).wait_recv()
    all_copies(FACTORS).wait_recv()
    for chip, c in partners:
        s = 2 * chip + c
        u_home[s, early] = b_send[s, early] + (
            factors[s, 0] * v_home[s, 0]
            + (factors[s, 1] * v_home[s, 1] + factors[s, 2] * v_home[s, 2])
        )
    rms_out[...] = jnp.broadcast_to(jnp.sqrt(total(2, RING) / cells), rms_out.shape)
    all_copies(LATE_ROWS).wait_recv()
    for kind in everything:
        all_copies(kind).wait_send()
    others(0, groups).wait_send()
    others(1, groups).wait_send()
    others(2, RING).wait_send()


def deliver(u, rms, u_out, rms_out, rms_row, sems):
    per = u.shape[0] // 1
    copies = [
        pltpu.make_async_copy(u.at[pl.ds(k * per, per)], u_out.at[pl.ds(k * per, per)], sems.at[k])
        for k in range(1)
    ]
    copies.append(pltpu.make_async_copy(rms_row, rms_out, sems.at[1]))
    for copy in copies[:-1]:
        copy.start()
    rms_row[...] = rms[0:1, 0:1]
    copies[-1].start()
    for copy in copies:
        copy.wait()


def shards(state, explicit_rhs, implicit_rhs, implicit_coef):
    species, _, ny, nx = state.shape
    sizes = (lax.axis_size(AXES[0]), lax.axis_size(AXES[1]))
    groups = sizes[0] * sizes[1]
    cells = species * ny * nx * groups * RING
    depth = RING + 2 * HALO
    f32 = jnp.float32
    hbm, vmem = (pl.BlockSpec(memory_space=m) for m in (pltpu.HBM, pltpu.VMEM))
    dma = pltpu.SemaphoreType.DMA
    u, rms = pl.pallas_call(
        functools.partial(kernel, sizes, cells),
        out_shape=(
            jax.ShapeDtypeStruct((species, ny, nx), f32),
            jax.ShapeDtypeStruct((8, 128), f32),
        ),
        in_specs=[hbm] * 4,
        out_specs=(vmem, vmem),
        scratch_shapes=[
            pltpu.VMEM((RING, ny, nx), f32),
            pltpu.VMEM((2, RING, ny, nx), f32),
            pltpu.VMEM((2, RING, ny, nx), f32),
            pltpu.SMEM((species,), f32),
            pltpu.VMEM((RING, ny, nx), f32),
            pltpu.VMEM((RING, ny, nx), f32),
            pltpu.VMEM((depth, ny, nx), f32),
            pltpu.VMEM((RING, ny, nx), f32),
            pltpu.VMEM((depth, ny, nx), f32),
            pltpu.VMEM((depth, ny, nx), f32),
            pltpu.VMEM((depth, ny, nx), f32),
            pltpu.VMEM((RING, 3, EARLY, nx), f32),
            pltpu.VMEM((RING, ny - EARLY, nx), f32),
            pltpu.VMEM((3, max(groups, RING), 1, 128), f32),
            pltpu.VMEM((3, 1, 128), f32),
            pltpu.VMEM((RING, 3, 1, nx), f32),
            dma((5,)),
            dma((RING,)),
            dma((2,)),
            dma((6,)),
            dma((6,)),
            dma((3,)),
            dma((3,)),
            pltpu.SemaphoreType.REGULAR((3,)),
        ],
        compiler_params=pltpu.CompilerParams(
            collective_id=0, has_side_effects=True, vmem_limit_bytes=24 * 2**20
        ),
        name="section",
    )(
        *(
            pltpu.with_memory_space_constraint(a, pltpu.HBM)
            for a in (state, explicit_rhs, implicit_rhs, implicit_coef)
        )
    )
    u, rms = pl.pallas_call(
        deliver,
        out_shape=(jax.ShapeDtypeStruct(u.shape, f32), jax.ShapeDtypeStruct((1, 1), f32)),
        in_specs=[vmem, vmem],
        out_specs=(hbm, hbm),
        scratch_shapes=[pltpu.VMEM((1, 1), f32), dma((2,))],
        compiler_params=pltpu.CompilerParams(vmem_limit_bytes=2**20),
        name="deliver",
    )(u, rms)
    return u.reshape(state.shape), rms[0, 0]


def solution(mesh):
    torus = Mesh(mesh.devices.reshape(-1, 8, 4, 2), AXES)
    placed = (
        P(None, AXES, None, None),
        P(None, None, AXES, None, None),
        P(None, None, AXES, None, None),
        P(),
    )
    return jax.shard_map(
        shards,
        mesh=torus,
        in_specs=placed,
        out_specs=(P(None, AXES, None, None), P()),
        check_vma=False,
    )
```

```python
import functools

import jax
import jax.numpy as jnp
from jax import lax
from jax.experimental import pallas as pl
from jax.experimental.pallas import tpu as pltpu
from jax.sharding import Mesh
from jax.sharding import PartitionSpec as P

AXES = ("gz_0", "gz_1", "gz_2", "gz_3")
MESH = pl.DeviceIdType.MESH

explicit_weights = (5535828885825.0 / 10492691773637.0, 788022342437.0 / 10882634858940.0)
implicit_weights = (2746238789719.0 / 10658868560708.0, -640167445237.0 / 6845629431997.0)

HALO = 4
RING = 8
MOMENTS = 6
SHIFT = 8.0
EARLY = 16


def remote(src, dst, send, recv, device):
    return pltpu.make_async_remote_copy(
        src_ref=src,
        dst_ref=dst,
        send_sem=send,
        recv_sem=recv,
        device_id=device,
        device_id_type=MESH,
    )


def laplace(below, here, above, shift=0.0):
    ny, nx = here.shape
    row = lax.broadcasted_iota(jnp.int32, here.shape, 0)
    lane = lax.broadcasted_iota(jnp.int32, here.shape, 1)
    beside = below + above
    beside = beside + jnp.where(row == ny - 1, 0.0, pltpu.roll(here, ny - 1, 0))
    beside = beside + jnp.where(row == 0, 0.0, pltpu.roll(here, 1, 0))
    beside = beside + jnp.where(lane == nx - 1, 0.0, pltpu.roll(here, nx - 1, 1))
    beside = beside + jnp.where(lane == 0, 0.0, pltpu.roll(here, 1, 1))
    return (6.0 - shift) * here - beside


def folded(value):
    total = value[0:8]
    for at in range(8, value.shape[0], 8):
        total = total + value[at : at + 8]
    return total


def row_of(sums):
    row = lax.broadcasted_iota(jnp.int32, (8, 128), 0)
    lane = lax.broadcasted_iota(jnp.int32, (8, 128), 1)
    stacked = jnp.zeros((8, 128), jnp.float32)
    for k, value in enumerate(sums):
        halves = sum(value[:, at : at + 128] for at in range(0, value.shape[1], 128))
        stacked = jnp.where(row == k, jnp.sum(halves, axis=0, keepdims=True), stacked)
    each = jnp.where(row == lane, jnp.sum(stacked, axis=1, keepdims=True), 0.0)
    return jnp.sum(each, axis=0, keepdims=True)


def entries(row, count):
    lane = lax.broadcasted_iota(jnp.int32, (1, 128), 1)
    return [
        jnp.sum(jnp.where(lane == k, row, 0.0), axis=1, keepdims=True) for k in range(count)
    ]


def basis_steps(nu, c):
    diagonal = 1.0 + SHIFT * c

    def gram(p, shift):
        total = None
        for i, a in enumerate(p):
            for j, b in enumerate(p):
                term = a * b * nu[i + j + shift]
                total = term if total is None else total + term
        return total

    def step(norm, along):
        energy = jnp.maximum(diagonal * gram(along, 0) + c * gram(along, 1), norm)
        return jnp.where(norm > 0.0, norm / energy, 0.0)

    norm = nu[0]
    first = norm / (diagonal * nu[0] + c * nu[1])
    residual = (1.0 - first * diagonal, -first * c)
    norm_next = jnp.maximum(gram(residual, 0), 0.0)
    ratio = norm_next / norm
    along = (residual[0] + ratio, residual[1])
    second = step(norm_next, along)
    norm = norm_next
    image = (diagonal * along[0], diagonal * along[1] + c * along[0], c * along[1])
    residual = (
        residual[0] - second * image[0],
        residual[1] - second * image[1],
        -second * image[2],
    )
    norm_next = jnp.maximum(gram(residual, 0), 0.0)
    ratio = jnp.where(norm > 0.0, norm_next / norm, 0.0)
    last = (residual[0] + ratio * along[0], residual[1] + ratio * along[1], residual[2])
    third = step(norm_next, last)
    return (
        -c * (first + second * along[0] + third * last[0]),
        -c * (second * along[1] + third * last[1]),
        -c * (third * last[2]),
    )


def kernel(
    sizes,
    cells,
    state,
    explicit,
    implicit,
    coef,
    u_home,
    rms_out,
    state_in,
    explicit_in,
    implicit_in,
    coef_in,
    b_send,
    d_send,
    field,
    weight,
    v0,
    v1,
    v2,
    v_home,
    u_send,
    rows,
    own_rows,
    factors,
    in_sem,
    b_recv,
    halo_recv,
    sent_sem,
    recv_sem,
    row_sent,
    row_recv,
    wave_sem,
):
    count_y, count_z = sizes
    groups = count_y * count_z
    ny = field.shape[1]
    y, z, x, core = (lax.axis_index(a) for a in AXES)
    place = 2 * x + core
    group = y * count_z + z
    right, left, across = lax.rem(x + 1, 4), lax.rem(x + 3, 4), lax.rem(x + 2, 4)

    flip = x // 2

    def in_ring(chip, c):
        return (y, z, chip, c)

    def layer(number, chip):
        turned = chip // 2
        return turned * (RING - 1) + (1 - 2 * turned) * number

    def at_group(step):
        of_group = lax.rem(group + step + groups, groups)
        return (of_group // count_z, lax.rem(of_group, count_z), x, core)

    def away(step_y, step_z):
        return (lax.rem(y + step_y, count_y), lax.rem(z + step_z + count_z, count_z), x, core)

    partner = (x, 1 - core)
    outside = [(chip, c) for c in (core, 1 - core) for chip in (across, right, left)]
    partners = [partner] + outside

    barrier = pltpu.get_barrier_semaphore()
    beside = [away(0, 1), away(0, -1), away(1, 0), away(count_y - 1, 0)]
    near = [in_ring(*p) for p in partners] + beside
    for device in near:
        pl.semaphore_signal(barrier, inc=1, device_id=device, device_id_type=MESH)

    for k, chip in enumerate((across, right, left, x)):
        pair = pl.ds(2 * chip, 2)
        for source, target in (
            (state.at[pair, 0], state_in.at[pair]),
            (explicit.at[:, pair, 0], explicit_in.at[:, pair]),
            (implicit.at[:, pair, 0], implicit_in.at[:, pair]),
        ):
            pltpu.make_async_copy(source, target, in_sem.at[k]).start()
    coef_load = pltpu.make_async_copy(coef, coef_in, in_sem.at[4])
    coef_load.start()

    def section_in(k, chip):
        ten = field.at[pl.ds(0, 10)]
        pltpu.make_async_copy(ten, ten, in_sem.at[k]).wait()
        for s in (2 * chip, 2 * chip + 1):
            b = (
                state_in[s]
                + explicit_weights[0] * explicit_in[0, s]
                + explicit_weights[1] * explicit_in[1, s]
            )
            b_send[s] = b + (
                implicit_weights[0] * implicit_in[0, s]
                + implicit_weights[1] * implicit_in[1, s]
            )

    BLOCK, HALO_BLOCK, WEIGHT, EARLY_ROWS, FACTORS, LATE_ROWS = range(6)

    def issue(source, target, kind, recv, device):
        remote(source, target, sent_sem.at[kind], recv, device).start()

    def some_copies(of, kind, recv):
        return remote(of, of, sent_sem.at[kind], recv, in_ring(right, core))

    def send_b(chip, c):
        issue(
            b_send.at[2 * chip + c],
            field.at[HALO + layer(place, chip)],
            BLOCK,
            b_recv.at[place],
            in_ring(chip, c),
        )

    def pass_on(number):
        origin = layer(number, x)
        half = origin // HALO

        @pl.when(origin != HALO)
        def _():
            issue(
                field.at[HALO + origin],
                field.at[lax.rem(origin + HALO + RING, HALO + RING + HALO)],
                HALO_BLOCK,
                halo_recv.at[1 - half],
                at_group((2 * half - 1) * (1 - 2 * flip)),
            )

    def b_arrived(chip, c):
        number = 2 * chip + c
        some_copies(field.at[HALO + layer(number, x)], BLOCK, b_recv.at[number]).wait_recv()
        return number

    section_in(0, across)
    pl.semaphore_wait(barrier, len(near))
    send_b(across, core)
    section_in(1, right)
    send_b(right, core)
    section_in(2, left)
    send_b(left, core)
    send_b(across, 1 - core)
    section_in(3, x)
    field[HALO + layer(place, x)] = b_send[place]
    send_b(*partner)
    send_b(right, 1 - core)
    send_b(left, 1 - core)

    waves = [beside, [away(0, k) for k in (1, -1, 2, -2)], [away(0, 2), away(0, -2)]]

    def wave(k):
        for device in waves[k]:
            pl.semaphore_signal(
                wave_sem.at[k], inc=1, device_id=device, device_id_type=MESH
            )

    def after_wave(k):
        pl.semaphore_wait(wave_sem.at[k], len(waves[k]))

    wave(0)

    def weigh(s, _):
        d = 1.0 / (1.0 + 0.1 * jnp.abs(state_in[s]))
        d_send[s] = d * d
        return _

    lax.fori_loop(0, RING, weigh, 0, unroll=2)
    weight[layer(place, x)] = d_send[place]
    after_wave(0)
    wave(1)
    pass_on(place)
    pass_on(b_arrived(*partner))
    for p in ((across, core), (right, core), (left, core), (across, 1 - core)):
        pass_on(b_arrived(*p))
    for chip, c in partners:
        number = 2 * chip + c
        issue(
            d_send.at[number],
            weight.at[layer(place, chip)],
            WEIGHT,
            recv_sem.at[WEIGHT],
            in_ring(chip, c),
        )
    for p in ((right, 1 - core), (left, 1 - core)):
        pass_on(b_arrived(*p))
    after_wave(1)
    wave(2)

    last = 2 * HALO + RING
    low, high = HALO, HALO + RING

    def planes(source, target, shift, start, stop):
        def body(j, _):
            target[j] = laplace(source[j - 1], source[j], source[j + 1], shift)
            return _

        lax.fori_loop(start, stop, body, 0, unroll=True)

    planes(field, v0, 0.0, low + 1, high - 1)
    planes(v0, v1, SHIFT, low + 2, high - 2)
    planes(v1, v2, SHIFT, low + 3, high - 3)
    zero = jnp.zeros((8, field.shape[-1]), jnp.float32)

    def moments(j, sums):
        a, b, e = v0[j], v1[j], v2[j]
        image = laplace(v2[j + 1], e, v2[j + 1], SHIFT)
        products = (a * a, a * b, b * b, b * e, e * e, e * image)
        return tuple(total + folded(product) for total, product in zip(sums, products))

    sums = (zero,) * MOMENTS
    middle = low + RING // 2
    for side, start, stop in (
        (1, lambda d: high - d, lambda d: last - d),
        (0, lambda d: d + 1, lambda d: low + d),
    ):
        blocks = field.at[pl.ds(1, 3) if side == 0 else pl.ds(high, HALO)]
        some_copies(blocks, HALO_BLOCK, halo_recv.at[side]).wait_recv()
        planes(field, v0, 0.0, start(1), stop(1))
        planes(v0, v1, SHIFT, start(2), stop(2))
        planes(v1, v2, SHIFT, start(3), stop(3))
        if side == 1:
            sums = lax.fori_loop(middle, high, moments, sums, unroll=True)

    for chip, c in outside + [partner]:
        number = 2 * chip + c
        for i, v in enumerate((v0, v1, v2)):
            issue(
                v.at[low + layer(number, x), pl.ds(0, EARLY)],
                v_home.at[place, i],
                EARLY_ROWS,
                recv_sem.at[EARLY_ROWS],
                in_ring(chip, c),
            )

    sums = lax.fori_loop(low, middle, moments, sums, unroll=True)

    far = sorted(
        ((dy, dz) for dy in range(count_y) for dz in range(count_z) if (dy, dz) != (0, 0)),
        key=lambda d: -min(d[0], count_y - d[0]) - min(d[1], count_z - d[1]),
    )

    def publish(phase, values):
        row = row_of(values)
        own_rows[phase] = row
        rows[phase, group] = row
        for step in far:
            remote(
                own_rows.at[phase],
                rows.at[phase, group],
                row_sent.at[phase],
                row_recv.at[phase],
                away(*step),
            ).start()

    def others(phase, count):
        some = rows.at[phase, pl.ds(0, count - 1)]
        return remote(
            some, some, row_sent.at[phase], row_recv.at[phase], in_ring(right, core)
        )

    def total(phase, count):
        others(phase, count).wait_recv()
        parts = [rows[phase, k] for k in range(count)]
        while len(parts) > 1:
            parts = [a + b for a, b in zip(parts[::2], parts[1::2])]
        return parts[0]

    after_wave(2)
    publish(0, sums)

    seven = pl.ds(0, RING - 1)
    everything = {
        BLOCK: b_send.at[seven],
        HALO_BLOCK: field.at[seven],
        WEIGHT: weight.at[seven],
        EARLY_ROWS: v_home.at[seven],
        FACTORS: factors.at[seven],
        LATE_ROWS: u_send.at[seven],
    }

    def all_copies(kind):
        return some_copies(everything[kind], kind, recv_sem.at[kind])

    all_copies(WEIGHT).wait_recv()

    def weighted(j, sums):
        d = weight[j - low]
        a, b, e = v0[j], v1[j], v2[j]
        da, db, de = d * a, d * b, d * e
        products = (da * a, da * b, da * e, db * b, db * e, de * e)
        return tuple(total + folded(product) for total, product in zip(sums, products))

    publish(1, lax.fori_loop(low, high, weighted, (zero,) * MOMENTS, unroll=2))
    coef_load.wait()

    c_here = coef_in[place]
    nu = entries(total(0, groups), MOMENTS)
    factor = basis_steps(nu, c_here)
    for i in range(3):
        factors[place, i] = jnp.broadcast_to(factor[i], factors.shape[2:])

    late = pl.ds(EARLY, ny - EARLY)

    def combined(k, of_rows):
        j = low + k
        return field[j, of_rows] + (
            factor[0] * v0[j, of_rows]
            + (factor[1] * v1[j, of_rows] + factor[2] * v2[j, of_rows])
        )

    def update(k, _):
        u_send[k] = combined(k, late)
        return _

    lax.fori_loop(0, RING, update, 0, unroll=2)
    for chip, c in partners:
        issue(
            factors.at[place],
            factors.at[place],
            FACTORS,
            recv_sem.at[FACTORS],
            in_ring(chip, c),
        )
    def send_u(*devices):
        for chip, c in devices:
            issue(
                u_send.at[layer(2 * chip + c, x)],
                u_home.at[place, late],
                LATE_ROWS,
                recv_sem.at[LATE_ROWS],
                in_ring(chip, c),
            )

    send_u((across, core), (right, core), (left, core), (across, 1 - core))

    g = entries(total(1, groups), MOMENTS)
    own = (
        factor[0] * factor[0] * g[0]
        + factor[1] * factor[1] * g[3]
        + factor[2] * factor[2] * g[5]
        + 2.0
        * (
            factor[0] * factor[1] * g[1]
            + factor[0] * factor[2] * g[2]
            + factor[1] * factor[2] * g[4]
        )
    )
    row = jnp.broadcast_to(own, (1, 128))
    own_rows[2] = row
    rows[2, place] = row
    for p in partners:
        remote(
            own_rows.at[2], rows.at[2, place], row_sent.at[2], row_recv.at[2], in_ring(*p)
        ).start()

    send_u((right, 1 - core), (left, 1 - core), partner)
    early = pl.ds(0, EARLY)
    mine = layer(place, x)
    u_home[place, late] = u_send[mine]
    u_home[place, early] = combined(mine, early)


    all_copies(EARLY_ROWS).wait_recv()
    all_copies(FACTORS).wait_recv()
    for chip, c in partners:
        s = 2 * chip + c
        u_home[s, early] = b_send[s, early] + (
            factors[s, 0] * v_home[s, 0]
            + (factors[s, 1] * v_home[s, 1] + factors[s, 2] * v_home[s, 2])
        )
    rms_out[...] = jnp.broadcast_to(jnp.sqrt(total(2, RING) / cells), rms_out.shape)
    all_copies(LATE_ROWS).wait_recv()
    for kind in everything:
        all_copies(kind).wait_send()
    others(0, groups).wait_send()
    others(1, groups).wait_send()
    others(2, RING).wait_send()


def deliver(u, rms, u_out, rms_out, rms_row, sems):
    per = u.shape[0] // 1
    copies = [
        pltpu.make_async_copy(u.at[pl.ds(k * per, per)], u_out.at[pl.ds(k * per, per)], sems.at[k])
        for k in range(1)
    ]
    copies.append(pltpu.make_async_copy(rms_row, rms_out, sems.at[1]))
    for copy in copies[:-1]:
        copy.start()
    rms_row[...] = rms[0:1, 0:1]
    copies[-1].start()
    for copy in copies:
        copy.wait()


def shards(state, explicit_rhs, implicit_rhs, implicit_coef):
    species, _, ny, nx = state.shape
    sizes = (lax.axis_size(AXES[0]), lax.axis_size(AXES[1]))
    groups = sizes[0] * sizes[1]
    cells = species * ny * nx * groups * RING
    depth = RING + 2 * HALO
    f32 = jnp.float32
    hbm, vmem = (pl.BlockSpec(memory_space=m) for m in (pltpu.HBM, pltpu.VMEM))
    dma = pltpu.SemaphoreType.DMA
    u, rms = pl.pallas_call(
        functools.partial(kernel, sizes, cells),
        out_shape=(
            jax.ShapeDtypeStruct((species, ny, nx), f32),
            jax.ShapeDtypeStruct((8, 128), f32),
        ),
        in_specs=[hbm] * 4,
        out_specs=(vmem, vmem),
        scratch_shapes=[
            pltpu.VMEM((RING, ny, nx), f32),
            pltpu.VMEM((2, RING, ny, nx), f32),
            pltpu.VMEM((2, RING, ny, nx), f32),
            pltpu.SMEM((species,), f32),
            pltpu.VMEM((RING, ny, nx), f32),
            pltpu.VMEM((RING, ny, nx), f32),
            pltpu.VMEM((depth, ny, nx), f32),
            pltpu.VMEM((RING, ny, nx), f32),
            pltpu.VMEM((depth, ny, nx), f32),
            pltpu.VMEM((depth, ny, nx), f32),
            pltpu.VMEM((depth, ny, nx), f32),
            pltpu.VMEM((RING, 3, EARLY, nx), f32),
            pltpu.VMEM((RING, ny - EARLY, nx), f32),
            pltpu.VMEM((3, max(groups, RING), 1, 128), f32),
            pltpu.VMEM((3, 1, 128), f32),
            pltpu.VMEM((RING, 3, 1, nx), f32),
            dma((5,)),
            dma((RING,)),
            dma((2,)),
            dma((6,)),
            dma((6,)),
            dma((3,)),
            dma((3,)),
            pltpu.SemaphoreType.REGULAR((3,)),
        ],
        compiler_params=pltpu.CompilerParams(
            collective_id=0, has_side_effects=True, vmem_limit_bytes=24 * 2**20
        ),
        name="section",
    )(
        *(
            pltpu.with_memory_space_constraint(a, pltpu.HBM)
            for a in (state, explicit_rhs, implicit_rhs, implicit_coef)
        )
    )
    u, rms = pl.pallas_call(
        deliver,
        out_shape=(jax.ShapeDtypeStruct(u.shape, f32), jax.ShapeDtypeStruct((1, 1), f32)),
        in_specs=[vmem, vmem],
        out_specs=(hbm, hbm),
        scratch_shapes=[pltpu.VMEM((1, 1), f32), dma((2,))],
        compiler_params=pltpu.CompilerParams(vmem_limit_bytes=2**20),
        name="deliver",
    )(u, rms)
    return u.reshape(state.shape), rms[0, 0]


def solution(mesh):
    torus = Mesh(mesh.devices.reshape(-1, 8, 4, 2), AXES)
    placed = (
        P(None, AXES, None, None),
        P(None, None, AXES, None, None),
        P(None, None, AXES, None, None),
        P(),
    )
    return jax.shard_map(
        shards,
        mesh=torus,
        in_specs=placed,
        out_specs=(P(None, AXES, None, None), P()),
        check_vma=False,
    )
```
